128 devices in a mesh: ty: 16 (over z, x), tx: 8 (over y, core).
Axes of the slice: x: 4, y: 4, z: 4, core: 2. Of those that a mesh axis runs over, the one named last changes fastest.
Arguments:
- fields: bfloat16 [2, 48, 128, 8192], P(None, None, 'ty', 'tx'), may hold values from -6 to 6
- kernel_one: bfloat16 [3, 3, 48, 32], replicated, may hold values from -0.3125 to 0.3125
- bias_one: float32 [32], replicated, may hold values from -1.5 to 1.5
- kernel_two: bfloat16 [3, 3, 32, 64], replicated, may hold values from -0.75 to 0.75
- bias_two: float32 [64], replicated, may hold values from -1.5 to 1.5
- kernel_three: bfloat16 [3, 3, 64, 128], replicated, may hold values from -0.5 to 0.5
- bias_three: float32 [128], replicated, may hold values from -1.5 to 1.5
- kernel_coarse: bfloat16 [3, 3, 128, 256], replicated, may hold values from -0.375 to 0.375
- bias_coarse: float32 [256], replicated, may hold values from -1.5 to 1.5
- decode_three: bfloat16 [3, 3, 384, 128], replicated, may hold values from -0.15625 to 0.15625
- offset_three: float32 [128], replicated, may hold values from -1.5 to 1.5
- decode_two: bfloat16 [3, 3, 192, 64], replicated, may hold values from -0.21875 to 0.21875
- offset_two: float32 [64], replicated, may hold values from -1.5 to 1.5
- decode_one: bfloat16 [3, 3, 96, 32], replicated, may hold values from -0.3125 to 0.3125
- offset_one: float32 [32], replicated, may hold values from -1.5 to 1.5
- head_kernel: bfloat16 [32, 48], replicated, may hold values from -1 to 1
- head_offset: float32 [48], replicated, may hold values from -3 to 3
Outputs:
- corrected: float32 [2, 48, 128, 8192], P(None, None, 'ty', 'tx')
The draws below stay inside these ranges and needn't reach their ends.
All inputs are finite; a program needn't handle non-finite values.
Results may differ from the reference program's by a relative error of at most 0.009.
Values may be sent and summed in bfloat16 or wider, within the bound.
No kernel may reach another device: no remote copies, remote signals or barrier semaphores. Data moves between devices by JAX's collectives and lax.ppermute only.
A program may use at most 128 MiB of HBM per device.

```python
import jax
import jax.numpy as jnp
from jax import lax

VARS = 48
C1 = 32
C2 = 64
C3 = 128
C4 = 256
HOURS = 2
NY = 128
NX = 8192


def steps_of(key, shape, shards, low, high):
    level, own = 1.0, jax.random.fold_in(key, 6)
    for axis_at, blocks in shards:
        heights = jnp.exp(jax.random.uniform(jax.random.fold_in(own, axis_at), (blocks,), jnp.float32, low / len(shards), high / len(shards)))
        level = level * jnp.repeat(heights, shape[axis_at] // blocks).reshape([-1 if axis == axis_at else 1 for axis in range(len(shape))])
    return level


def gaussian(rng, shape, deviation, limit, split=(), dtype=jnp.bfloat16):
    level = steps_of(rng, shape, split, -0.22, 0.18) if split else 1.0
    values = jax.random.normal(rng, shape, jnp.float32) * deviation * level
    return jnp.minimum(jnp.maximum(values, -limit), limit).astype(dtype)


def setup_inputs(seed: int = 0) -> dict:
    splits = jax.random.split(jax.random.key(seed), 18)
    fields = gaussian(splits[0], (HOURS, VARS, NY, NX), 1.0, 6.0, ((2, 16), (3, 8)))
    kernel_one = gaussian(splits[1], (3, 3, VARS, C1), (9 * VARS) ** -0.5, 0.3125)
    bias_one = gaussian(splits[2], (C1,), 0.25, 1.5, (), jnp.float32)
    kernel_two = gaussian(splits[3], (3, 3, C1, C2), (2 * C1) ** -0.5, 0.75)
    bias_two = gaussian(splits[4], (C2,), 0.25, 1.5, (), jnp.float32)
    kernel_three = gaussian(splits[5], (3, 3, C2, C3), (2 * C2) ** -0.5, 0.5)
    bias_three = gaussian(splits[6], (C3,), 0.25, 1.5, (), jnp.float32)
    kernel_coarse = gaussian(splits[7], (3, 3, C3, C4), (2 * C3) ** -0.5, 0.375)
    bias_coarse = gaussian(splits[8], (C4,), 0.25, 1.5, (), jnp.float32)
    decode_three = gaussian(splits[9], (3, 3, C4 + C3, C3), (4 * (C4 + C3)) ** -0.5, 0.15625)
    offset_three = gaussian(splits[10], (C3,), 0.25, 1.5, (), jnp.float32)
    decode_two = gaussian(splits[11], (3, 3, C3 + C2, C2), (4 * (C3 + C2)) ** -0.5, 0.21875)
    offset_two = gaussian(splits[12], (C2,), 0.25, 1.5, (), jnp.float32)
    decode_one = gaussian(splits[13], (3, 3, C2 + C1, C1), (4 * (C2 + C1)) ** -0.5, 0.3125)
    offset_one = gaussian(splits[14], (C1,), 0.25, 1.5, (), jnp.float32)
    head_kernel = gaussian(splits[15], (C1, VARS), C1 ** -0.5, 1.0)
    head_offset = gaussian(splits[16], (VARS,), 0.5, 3.0, (), jnp.float32)
    return dict(fields=fields, kernel_one=kernel_one, bias_one=bias_one, kernel_two=kernel_two, bias_two=bias_two, kernel_three=kernel_three, bias_three=bias_three, kernel_coarse=kernel_coarse, bias_coarse=bias_coarse, decode_three=decode_three, offset_three=offset_three, decode_two=decode_two, offset_two=offset_two, decode_one=decode_one, offset_one=offset_one, head_kernel=head_kernel, head_offset=head_offset)


def convolve(tensor, kernel, offset):
    result = lax.conv_general_dilated(tensor, kernel, (1, 1), ((1, 1), (1, 1)), dimension_numbers=("NCHW", "HWIO", "NCHW"), preferred_element_type=jnp.float32)
    return jax.nn.silu(result + offset[None, :, None, None]).astype(jnp.bfloat16)


def average_pool(tensor):
    shape = tensor.shape
    blocks = tensor.astype(jnp.float32).reshape(shape[0], shape[1], shape[2] // 2, 2, shape[3] // 2, 2)
    return jnp.mean(blocks, axis=(3, 5)).astype(jnp.bfloat16)


def upsample(tensor):
    return jnp.repeat(jnp.repeat(tensor, 2, axis=2), 2, axis=3)


def reference(fields, kernel_one, bias_one, kernel_two, bias_two, kernel_three, bias_three, kernel_coarse, bias_coarse, decode_three, offset_three, decode_two, offset_two, decode_one, offset_one, head_kernel, head_offset):
    skip_one = convolve(fields, kernel_one, bias_one)
    skip_two = convolve(average_pool(skip_one), kernel_two, bias_two)
    skip_three = convolve(average_pool(skip_two), kernel_three, bias_three)
    coarse = convolve(average_pool(skip_three), kernel_coarse, bias_coarse)
    back_three = convolve(jnp.concatenate([upsample(coarse), skip_three], axis=1), decode_three, offset_three)
    back_two = convolve(jnp.concatenate([upsample(back_three), skip_two], axis=1), decode_two, offset_two)
    back_one = convolve(jnp.concatenate([upsample(back_two), skip_one], axis=1), decode_one, offset_one)
    projected = jnp.einsum("bchw,cv->bvhw", back_one.astype(jnp.float32), head_kernel.astype(jnp.float32), precision=lax.Precision.HIGHEST)
    return fields.astype(jnp.float32) + head_offset[None, :, None, None] + projected
```

```python
import jax
import jax.numpy as jnp
from jax import lax
from jax.experimental import pallas as pl
from jax.experimental.pallas import tpu as pltpu
from jax.sharding import PartitionSpec as P

LANES = 128
WIDE = 384
BF16 = jnp.bfloat16
F32 = jnp.float32


def neighbour(value, axis, step):
    size = lax.axis_size(axis)
    return lax.ppermute(value, axis, [(i, (i + step) % size) for i in range(size)])


def call(body, name, out_shapes, scratch, args, limit=16):
    specs = [pl.BlockSpec(memory_space=pltpu.VMEM)] * len(args)
    return pl.pallas_call(
        body,
        name=name,
        out_shape=[jax.ShapeDtypeStruct(s, d) for s, d in out_shapes],
        in_specs=specs,
        out_specs=[pl.BlockSpec(memory_space=pltpu.VMEM)] * len(out_shapes),
        scratch_shapes=scratch,
        compiler_params=pltpu.CompilerParams(vmem_limit_bytes=limit * 2**20),
    )(*args)


def iota(shape, axis):
    return lax.broadcasted_iota(jnp.int32, shape, axis)


def edges():
    ty, tx = lax.axis_index("ty"), lax.axis_index("tx")
    ny, nx = lax.axis_size("ty"), lax.axis_size("tx")
    inside = (ty > 0, ty < ny - 1, tx > 0, tx < nx - 1)
    return [jnp.where(side, 1.0, 0.0) for side in inside]


def one_hot(cond):
    return jnp.where(cond, 1.0, 0.0).astype(BF16)


def dot(a, b):
    return jnp.dot(a, b, preferred_element_type=F32)


def silu(t):
    return t * (0.5 * jnp.tanh(0.5 * t) + 0.5)


def lane_mask(flags):
    lane = iota((1, WIDE), 1)
    place = lane & 15
    edge = lane >= 256
    left = jnp.where(edge & (place < 4), flags[2], 1.0)
    right = jnp.where(edge & (place >= 12), flags[3], 1.0)
    return left * right


def from_left(slab):
    lane = iota((1, LANES), 1)
    h0, h1, edge = slab[:, :128], slab[:, 128:256], slab[:, 256:]
    h0 = jnp.where(lane == 0, pltpu.roll(edge, 125, 1), pltpu.roll(h0, 1, 1))
    h1 = jnp.where(lane == 0, pltpu.roll(edge, 109, 1), pltpu.roll(h1, 1, 1))
    return jnp.concatenate([h0, h1, pltpu.roll(edge, 1, 1)], axis=1)


def from_right(slab):
    lane = iota((1, LANES), 1)
    h0, h1, edge = slab[:, :128], slab[:, 128:256], slab[:, 256:]
    h0 = jnp.where(lane == 127, pltpu.roll(edge, 115, 1), pltpu.roll(h0, 127, 1))
    h1 = jnp.where(lane == 127, pltpu.roll(edge, 99, 1), pltpu.roll(h1, 127, 1))
    return jnp.concatenate([h0, h1, pltpu.roll(edge, 127, 1)], axis=1)


def put(scratch, row, phases, slab_of, valid=None):
    for p in range(phases):
        slab = slab_of(p)
        if valid is not None:
            slab = jnp.where(valid > 0.5, slab, jnp.zeros_like(slab))
        scratch[row, p + 1] = slab
        if p == 0:
            scratch[row, phases + 1] = from_right(slab)
        if p == phases - 1:
            scratch[row, 0] = from_left(slab)


def window(scratch, row, phase, rows, cols):
    v = scratch[pl.ds(row, rows), phase : phase + cols]
    return v.reshape(rows * cols * v.shape[2], v.shape[3])


def fields_kernel(x, fl, fr, out):
    flags = edges()
    lane = iota((1, LANES), 1)
    rows = x.shape[1]
    i, k = iota((rows, rows), 0), iota((rows, rows), 1)
    turn = one_hot(i == (k & 7) * (rows // 8) + (k >> 3))
    ends = []
    for h in range(2):
        a = jnp.where((lane >= 96) & (flags[2] > 0.5), fl[h], jnp.where(lane < 32, x[h, :, :128], 0))
        b = jnp.where(lane >= 96, x[h, :, 896:], jnp.where((lane < 32) & (flags[3] > 0.5), fr[h], 0))
        ends += [a.astype(BF16), b.astype(BF16)]
    ends = jnp.concatenate(ends, axis=1)
    channels = rows // 8
    for q in range(4):
        c = iota((1, 256), 1)
        split = one_hot(iota((1024, 256), 0) == 8 * (c & 127) + 2 * q + (c >> 7))
        row = 128 * ((c & 127) >> 3) + (((8 * (c & 7) + 2 * q + (c >> 7)) + 96) & 127)
        pick = (iota((512, 256), 0) == row) & ((c & 127) < 32)
        parts = [dot(x[0], split), dot(x[1], split), dot(ends, one_hot(pick))]
        for n, part in enumerate(parts):
            part = dot(turn, part.astype(BF16)).astype(BF16)
            for r in range(8):
                for s in range(2):
                    out[r, 2 * q + s, :, n * 128 : (n + 1) * 128] = part[
                        r * channels : (r + 1) * channels, s * 128 : (s + 1) * 128
                    ]


def one_kernel(x, above, below, w, b, skip, pooled, first, last, xs):
    flags = edges()
    put(xs, 0, 8, lambda p: above[p], flags[0])
    for r in range(8):
        put(xs, r + 1, 8, lambda p: x[r, p])
    put(xs, 9, 8, lambda p: below[p], flags[1])
    mask = lane_mask(flags)
    bias = b[...]

    def pair(k, carry):
        for q in range(4):
            total = None
            for r in range(2):
                rhs = jnp.concatenate(
                    [window(xs, 2 * k + r, 2 * q + s, 3, 3) for s in range(2)], axis=1
                )
                res = dot(w[...], rhs)
                for s in range(2):
                    y = (silu(res[:, s * WIDE : (s + 1) * WIDE] + bias) * mask).astype(BF16)
                    skip[2 * k + r, 2 * q + s] = y
                    total = y.astype(F32) if total is None else total + y.astype(F32)
            pooled[k, q] = (total * 0.25).astype(BF16)
        return carry

    lax.fori_loop(0, 4, pair, 0)
    first[...] = pooled[0:3]
    last[...] = pooled[1:4]


def two_kernel(x, above, below, w2, b2, w3, b3, skip2, skip3, coarse_in, xs, xs3, tmp):
    flags = edges()
    for r in range(3):
        put(xs, r, 4, lambda p: above[r, p], flags[0])
        put(xs, r + 7, 4, lambda p: below[r, p], flags[1])
    for r in range(4):
        put(xs, r + 3, 4, lambda p: x[r, p])
    mask = lane_mask(flags)
    bias = b2[...]

    def pair(k, carry):
        valid = jnp.where(k == 0, flags[0], jnp.where(k == 3, flags[1], 1.0))
        for q in range(2):
            total = None
            for r in range(2):
                rhs = jnp.concatenate(
                    [window(xs, 2 * k + r, 2 * q + s, 3, 3) for s in range(2)], axis=1
                )
                res = dot(w2[...], rhs)
                for s in range(2):
                    y = silu(res[:, s * WIDE : (s + 1) * WIDE] + bias) * (mask * valid)
                    y = y.astype(BF16)
                    skip2[2 * k + r, 2 * q + s] = y
                    total = y.astype(F32) if total is None else total + y.astype(F32)
            tmp[k, q] = (total * 0.25).astype(BF16)
        return carry

    lax.fori_loop(0, 4, pair, 0)
    for r in range(4):
        put(xs3, r, 2, lambda p: tmp[r, p])
    total = None
    for r in range(2):
        for p in range(2):
            y = silu(dot(w3[...], window(xs3, r, p, 3, 3)) + b3[...]) * mask
            y = y.astype(BF16)
            skip3[r, p] = y
            total = y.astype(F32) if total is None else total + y.astype(F32)
    coarse_in[...] = (total * 0.25).astype(BF16)


def coarse_kernel(x, above, below, w, b, out, xs):
    flags = edges()
    put(xs, 0, 1, lambda p: above[...], flags[0])
    put(xs, 1, 1, lambda p: x[...])
    put(xs, 2, 1, lambda p: below[...], flags[1])
    res = dot(w[...], window(xs, 0, 0, 3, 3)) + b[...]
    out[...] = (silu(res) * lane_mask(flags)).astype(BF16)


def back_kernel(
    c, c_up, c_dn, s3, s3_up, s3_dn, s2, wu3, ws3, b3, wu2, ws2, b2, out, xc, x3, xb, x2
):
    flags = edges()
    put(xc, 0, 1, lambda p: c_up[...], flags[0])
    put(xc, 1, 1, lambda p: c[...])
    put(xc, 2, 1, lambda p: c_dn[...], flags[1])
    for r in range(2):
        put(x3, r, 2, lambda p: s3_up[r, p], flags[0])
        put(x3, r + 2, 2, lambda p: s3[r, p])
        put(x3, r + 4, 2, lambda p: s3_dn[r, p], flags[1])
    mask = lane_mask(flags)
    for r in range(-1, 3):
        valid = flags[0] if r < 0 else flags[1] if r > 1 else None
        slabs = []
        for p in range(2):
            res = dot(wu3[r & 1, p], window(xc, (r + 1) // 2, p, 2, 2))
            res = res + dot(ws3[...], window(x3, r + 1, p, 3, 3))
            y = silu(res + b3[...]) * mask
            if valid is not None:
                y = y * valid
            slabs.append(y.astype(BF16))
        put(xb, r + 1, 2, lambda p: slabs[p])
    for r in range(8):
        put(x2, r, 4, lambda p: s2[r, p])

    def pair(k, carry):
        for i in range(2):
            valid = jnp.where(
                (k == 0) & (i == 0), flags[0], jnp.where((k == 2) & (i == 1), flags[1], 1.0)
            )
            for p in range(4):
                res = dot(wu2[1 - i, p & 1], window(xb, k, (p + 1) // 2, 2, 2))
                res = res + dot(ws2[...], window(x2, 2 * k + i, p, 3, 3))
                out[2 * k + i, p] = (silu(res + b2[...]) * (mask * valid)).astype(BF16)
        return carry

    lax.fori_loop(0, 3, pair, 0)


def last_kernel(bt, s1, s1_up, s1_dn, wu, ws, b, out, xb, x1):
    flags = edges()
    for r in range(6):
        put(xb, r, 4, lambda p: bt[r, p])
    put(x1, 0, 8, lambda p: s1_up[p], flags[0])
    for r in range(8):
        put(x1, r + 1, 8, lambda p: s1[r, p])
    put(x1, 9, 8, lambda p: s1_dn[p], flags[1])

    def pair(k, carry):
        for i in range(2):
            for p in range(8):
                up = window(xb, k + i, (p + 1) // 2, 2, 2)[:, :256]
                res = dot(wu[i, p & 1], up)
                res = res + dot(ws[...], window(x1, 2 * k + i, p, 3, 3)[:, :256])
                y = silu(res + b[...]).astype(BF16)
                for h in range(2):
                    out[h, 2 * k + i, :, p * 128 : (p + 1) * 128] = y[:, h * 128 : (h + 1) * 128]
        return carry

    lax.fori_loop(0, 4, pair, 0)


def head_kernel_body(back, fields, w, offset, out):
    col = iota((1, 256), 1) + 256 * pl.program_id(0)
    merge = one_hot(iota((1024, 256), 0) == 128 * (col & 7) + (col >> 3))
    for h in range(2):
        rows = dot(back[h], merge).astype(BF16)
        out[h] = fields[h].astype(F32) + offset[...] + dot(w[...], rows)


def flip(value):
    eye = one_hot(iota((value.shape[1],) * 2, 0) == iota((value.shape[1],) * 2, 1))
    dims = (((1,), (1,)), ((), ()))
    return lax.dot_general(eye, value, dims, preferred_element_type=F32).astype(BF16)


def column(row, width, repeat=1):
    size = row.shape[1]
    i, j = iota((size * repeat, size), 0), iota((size * repeat, size), 1)
    col = jnp.sum(jnp.where(i // repeat == j, row, 0.0), axis=1, keepdims=True)
    return jnp.broadcast_to(col, (size * repeat, width))


def sums(a):
    return ((0,), (1, 2)) if a == 0 else ((0, 1), (2,))


def summed(tap, a, b, i, j):
    total = None
    for dy in sums(a)[i]:
        for dx in sums(b)[j]:
            value = tap(dy, dx).astype(F32)
            total = value if total is None else total + value
    return total.astype(BF16)


def placed(parts, width):
    size = parts[0].shape[1]
    total = None
    for n, part in enumerate(parts):
        spot = one_hot(iota((size, width), 1) == iota((size, width), 0) + n * size)
        value = dot(part, spot)
        total = value if total is None else total + value
    return total.astype(BF16)


NINE = [(dy, dx) for dy in range(3) for dx in range(3)]
FOUR = [(i, j) for i in range(2) for j in range(2)]


def early_kernel(k1, k2, k3, r1, r2, r3, w1, w2, w3, b1, b2, b3):
    w1[...] = placed([k1[n] for n in NINE], w1.shape[1])
    w2[...] = flip(k2[...].reshape(-1, k2.shape[3]))
    w3[...] = flip(k3[...].reshape(-1, k3.shape[3]))
    for r, b in ((r1, b1), (r2, b2), (r3, b3)):
        b[...] = column(r[...], WIDE)


def late_kernel(
    kc, d3, d2, d1, hk, rc, r3, r2, r1, rh, wc, wu3, ws3, wu2, ws2, wu1, ws1, wh, bc, b3, b2, b1, bh
):
    wc[...] = flip(kc[...].reshape(-1, kc.shape[3]))
    for r, b in ((rc, bc), (r3, b3), (r2, b2), (r1, b1)):
        b[...] = column(r[...], b.shape[1])
    bh[...] = column(rh[...], bh.shape[1], 8)
    up3, up2, up1 = wu3.shape[3] // 4, wu2.shape[3] // 4, wu1.shape[3] // 4
    for a in range(2):
        for b in range(2):
            tall = [summed(lambda y, x: d3[y, x, :up3, :], a, b, i, j) for i, j in FOUR]
            wu3[a, b] = flip(jnp.concatenate(tall, axis=0))
            wide = [summed(lambda y, x: d2[y, x, :, :up2], a, b, i, j) for i, j in FOUR]
            wu2[a, b] = jnp.concatenate(wide, axis=1)
            wide = [summed(lambda y, x: d1[y, x, :, :up1], a, b, i, j) for i, j in FOUR]
            wu1[a, b] = placed(wide, wu1.shape[3])
    ws3[...] = flip(jnp.concatenate([d3[y, x, up3:, :] for y, x in NINE], axis=0))
    ws2[...] = placed([d2[y, x, :, up2:] for y, x in NINE], ws2.shape[1])
    ws1[...] = placed([d1[y, x, :, up1:] for y, x in NINE], ws1.shape[1])
    v, c = hk.shape[1], hk.shape[0]
    spread = one_hot(iota((v * 8, v), 0) // 8 == iota((v * 8, v), 1))
    dims = (((1,), (1,)), ((), ()))
    tall = lax.dot_general(spread, hk[...], dims, preferred_element_type=F32).astype(BF16)
    i, k = iota((v * 8, 8 * c), 0), iota((v * 8, 8 * c), 1)
    tiled = dot(tall, one_hot(iota((c, 8 * c), 0) == iota((c, 8 * c), 1) % c))
    wh[...] = jnp.where(i % 8 == k // c, tiled, 0.0).astype(BF16)


def body(
    fields,
    kernel_one,
    bias_one,
    kernel_two,
    bias_two,
    kernel_three,
    bias_three,
    kernel_coarse,
    bias_coarse,
    decode_three,
    offset_three,
    decode_two,
    offset_two,
    decode_one,
    offset_one,
    head_kernel,
    head_offset,
):
    c1, c2, c3, c4 = (k.shape[3] for k in (kernel_one, kernel_two, kernel_three, kernel_coarse))
    v = fields.shape[1]

    x = fields.reshape(2, v * 8, 1024)
    from_l = neighbour(x[:, :, 896:], "tx", 1)
    from_r = neighbour(x[:, :, :128], "tx", -1)

    def up(value):
        return neighbour(value, "ty", -1)

    def down(value):
        return neighbour(value, "ty", 1)

    row = lambda bias: bias[None, :]
    swap = lambda kernel: jnp.transpose(kernel, (0, 1, 3, 2))
    weights = lambda *shape: (shape, BF16)
    biases = lambda size, width=WIDE: ((size, width), F32)
    w1, w2, w3, b1, b2, b3 = call(
        early_kernel,
        "early",
        [weights(c1, 9 * v), weights(c2, 9 * c1), weights(c3, 9 * c2)]
        + [biases(c1), biases(c2), biases(c3)],
        [],
        [swap(kernel_one), kernel_two, kernel_three, row(bias_one), row(bias_two), row(bias_three)],
    )
    wc, wu3, ws3, wu2, ws2, wu1, ws1, wh, bc, ob3, ob2, ob1, bh = call(
        late_kernel,
        "late",
        [weights(c4, 9 * c3), weights(2, 2, c3, 4 * c4), weights(c3, 9 * c3)]
        + [weights(2, 2, c2, 4 * c3), weights(c2, 9 * c2)]
        + [weights(2, 2, c1, 4 * c2), weights(c1, 9 * c1), weights(8 * v, 8 * c1)]
        + [biases(c4), biases(c3), biases(c2), biases(c1, 256), biases(8 * v, 256)],
        [],
        [kernel_coarse, decode_three, swap(decode_two), swap(decode_one), head_kernel]
        + [row(b) for b in (bias_coarse, offset_three, offset_two, offset_one, head_offset)],
    )
    (f,) = call(fields_kernel, "fields", [((8, 8, v, WIDE), BF16)], [], [x, from_l, from_r])
    s1, p1, p1_first, p1_last = call(
        one_kernel,
        "one",
        [((8, 8, c1, WIDE), BF16), ((4, 4, c1, WIDE), BF16)] + [((3, 4, c1, WIDE), BF16)] * 2,
        [pltpu.VMEM((10, 10, v, WIDE), BF16)],
        [f, down(f[7]), up(f[0]), w1, b1],
    )
    s2, s3, coarse_in = call(
        two_kernel,
        "two",
        [((8, 4, c2, WIDE), BF16), ((2, 2, c3, WIDE), BF16), ((c3, WIDE), BF16)],
        [
            pltpu.VMEM((10, 6, c1, WIDE), BF16),
            pltpu.VMEM((4, 4, c2, WIDE), BF16),
            pltpu.VMEM((4, 2, c2, WIDE), BF16),
        ],
        [p1, down(p1_last), up(p1_first), w2, b2]
        + [w3, b3],
    )
    (coarse,) = call(
        coarse_kernel,
        "coarse",
        [((c4, WIDE), BF16)],
        [pltpu.VMEM((3, 3, c3, WIDE), BF16)],
        [coarse_in, down(coarse_in), up(coarse_in), wc, bc],
    )
    (back_two,) = call(
        back_kernel,
        "back",
        [((6, 4, c2, WIDE), BF16)],
        [
            pltpu.VMEM((3, 3, c4, WIDE), BF16),
            pltpu.VMEM((6, 4, c3, WIDE), BF16),
            pltpu.VMEM((4, 4, c3, WIDE), BF16),
            pltpu.VMEM((8, 6, c2, WIDE), BF16),
        ],
        [coarse, down(coarse), up(coarse), s3, down(s3), up(s3), s2]
        + [wu3, ws3, ob3, wu2, ws2, ob2],
    )
    (back_one,) = call(
        last_kernel,
        "last",
        [((2, 8, c1, 1024), BF16)],
        [pltpu.VMEM((6, 6, c2, WIDE), BF16), pltpu.VMEM((10, 10, c1, WIDE), BF16)],
        [back_two, s1, down(s1[7]), up(s1[0])]
        + [wu1, ws1, ob1],
    )
    block = lambda rows, dtype: pl.BlockSpec((2, rows, 256), lambda i: (0, 0, i))
    whole = lambda *shape: pl.BlockSpec(shape, lambda i: (0,) * len(shape))
    out = pl.pallas_call(
        head_kernel_body,
        name="head",
        grid=(4,),
        out_shape=jax.ShapeDtypeStruct((2, v * 8, 1024), F32),
        in_specs=[whole(2, 8 * c1, 1024), block(v * 8, BF16), whole(v * 8, 8 * c1), whole(v * 8, 256)],
        out_specs=block(v * 8, F32),
        compiler_params=pltpu.CompilerParams(vmem_limit_bytes=24 * 2**20),
    )(
        back_one.reshape(2, 8 * c1, 1024),
        x,
        wh,
        bh,
    )
    return out.reshape(2, v, 8, 1024)


def solution(mesh):
    return jax.shard_map(
        body,
        mesh=mesh,
        in_specs=(P(None, None, "ty", "tx"),) + (P(),) * 16,
        out_specs=P(None, None, "ty", "tx"),
        check_vma=False,
    )
```

```python
import jax
import jax.numpy as jnp
from jax import lax
from jax.experimental import pallas as pl
from jax.experimental.pallas import tpu as pltpu
from jax.sharding import PartitionSpec as P

LANES = 128
WIDE = 384
BF16 = jnp.bfloat16
F32 = jnp.float32


def neighbour(value, axis, step):
    size = lax.axis_size(axis)
    return lax.ppermute(value, axis, [(i, (i + step) % size) for i in range(size)])


def call(body, name, out_shapes, scratch, args, limit=16, flops=0):
    specs = [pl.BlockSpec(memory_space=pltpu.VMEM)] * len(args)
    return pl.pallas_call(
        body,
        name=name,
        out_shape=[jax.ShapeDtypeStruct(s, d) for s, d in out_shapes],
        in_specs=specs,
        out_specs=[pl.BlockSpec(memory_space=pltpu.VMEM)] * len(out_shapes),
        scratch_shapes=scratch,
        cost_estimate=pl.CostEstimate(flops=flops, transcendentals=0, bytes_accessed=0),
        compiler_params=pltpu.CompilerParams(vmem_limit_bytes=limit * 2**20),
    )(*args)


def iota(shape, axis):
    return lax.broadcasted_iota(jnp.int32, shape, axis)


def edges():
    ty, tx = lax.axis_index("ty"), lax.axis_index("tx")
    ny, nx = lax.axis_size("ty"), lax.axis_size("tx")
    inside = (ty > 0, ty < ny - 1, tx > 0, tx < nx - 1)
    return [jnp.where(side, 1.0, 0.0) for side in inside]


def one_hot(cond):
    return jnp.where(cond, 1.0, 0.0).astype(BF16)


def dot(a, b):
    return jnp.dot(a, b, preferred_element_type=F32)


def silu(t):
    return t * (0.5 * jnp.tanh(0.5 * t) + 0.5)


def lane_mask(flags):
    lane = iota((1, WIDE), 1)
    place = lane & 15
    edge = lane >= 256
    left = jnp.where(edge & (place < 4), flags[2], 1.0)
    right = jnp.where(edge & (place >= 12), flags[3], 1.0)
    return left * right


def from_left(slab):
    lane = iota((1, LANES), 1)
    h0, h1, edge = slab[:, :128], slab[:, 128:256], slab[:, 256:]
    h0 = jnp.where(lane == 0, pltpu.roll(edge, 125, 1), pltpu.roll(h0, 1, 1))
    h1 = jnp.where(lane == 0, pltpu.roll(edge, 109, 1), pltpu.roll(h1, 1, 1))
    return jnp.concatenate([h0, h1, pltpu.roll(edge, 1, 1)], axis=1)


def from_right(slab):
    lane = iota((1, LANES), 1)
    h0, h1, edge = slab[:, :128], slab[:, 128:256], slab[:, 256:]
    h0 = jnp.where(lane == 127, pltpu.roll(edge, 115, 1), pltpu.roll(h0, 127, 1))
    h1 = jnp.where(lane == 127, pltpu.roll(edge, 99, 1), pltpu.roll(h1, 127, 1))
    return jnp.concatenate([h0, h1, pltpu.roll(edge, 127, 1)], axis=1)


def fill(scratch, row, slabs, valid=None):
    phases = len(slabs)
    for p, slab in enumerate(slabs):
        if valid is not None:
            slab = jnp.where(valid > 0.5, slab, jnp.zeros_like(slab))
        scratch[row, p + 1] = slab
        if p == 0:
            scratch[row, phases + 1] = from_right(slab)
        if p == phases - 1:
            scratch[row, 0] = from_left(slab)


def window(scratch, row, phase, rows, cols):
    v = scratch[pl.ds(row, rows), phase : phase + cols]
    return v.reshape(rows * cols * v.shape[2], v.shape[3])


def side(*parts):
    return jnp.concatenate(parts, axis=1)


def pack(out, slabs):
    lane = iota((1, LANES), 1)
    count = len(slabs)
    for n, slab in enumerate(slabs):
        out[2 * n] = slab[:, :128]
        out[2 * n + 1] = slab[:, 128:256]
    for g in range(0, count, 4):
        tile = slabs[g][:, 256:]
        for n in range(1, min(4, count - g)):
            tile = jnp.where(lane < 32 * n, tile, pltpu.roll(slabs[g + n][:, 256:], 32 * n, 1))
        out[2 * count + g // 4] = tile


def unpack(packed, n, count):
    tile = packed[2 * count + n // 4]
    if n % 4:
        tile = pltpu.roll(tile, 128 - 32 * (n % 4), 1)
    return side(packed[2 * n], packed[2 * n + 1], tile)


def tiles(count):
    return 2 * count + (count + 3) // 4


def turned(part):
    rows = part.shape[0]
    i, k = iota((rows, rows), 0), iota((rows, rows), 1)
    turn = one_hot(i == (k & 7) * (rows // 8) + (k >> 3))
    return dot(turn, part).astype(BF16)


def main_kernel(x, out):
    channels = x.shape[1] // 8
    lane = iota((1, LANES), 1)
    c = iota((1, 256), 1)
    split = one_hot(iota((256, 256), 0) == 8 * (c & 31) + (c >> 5))
    for h in range(2):
        blocks = [dot(x[h, :, q * 256 : (q + 1) * 256], split).astype(BF16) for q in range(4)]
        phases = []
        for p in range(8):
            half = slice((p // 4) * 128, (p // 4 + 1) * 128)
            tile = rolled(blocks[0][:, half], -32 * (p % 4))
            for q in range(1, 4):
                tile = jnp.where(lane < 32 * q, tile, rolled(blocks[q][:, half], 32 * (q - p % 4)))
            phases.append(tile)
        for q in range(4):
            part = turned(side(phases[2 * q], phases[2 * q + 1]))
            for r in range(8):
                rows = part[r * channels : (r + 1) * channels]
                for s in range(2):
                    out[r, 2 * q + s, :, h * 128 : (h + 1) * 128] = rows[:, s * 128 : (s + 1) * 128]


def rolled(value, shift):
    return pltpu.roll(value, shift % 128, 1) if shift % 128 else value


def ends_kernel(x, main, fl, fr, out, first, last):
    flags = edges()
    lane = iota((1, LANES), 1)
    channels = x.shape[1] // 8
    ends = []
    for h in range(2):
        a = jnp.where((lane >= 96) & (flags[2] > 0.5), fl[h], jnp.where(lane < 32, x[h, :, :128], 0))
        b = jnp.where(lane >= 96, x[h, :, 896:], jnp.where((lane < 32) & (flags[3] > 0.5), fr[h], 0))
        ends += [a.astype(BF16), b.astype(BF16)]
    ends = side(*ends)
    c = iota((1, 256), 1)
    row = 128 * ((c & 31) >> 3) + (((8 * (c & 7) + (c >> 5)) + 96) & 127)
    part = turned(dot(ends, one_hot(iota((512, 256), 0) == row)).astype(BF16))
    for r in range(8):
        rows = part[r * channels : (r + 1) * channels]
        for p in range(8):
            tile = rows[:, (p // 4) * 128 : (p // 4 + 1) * 128]
            out[r, p] = pltpu.roll(tile, 128 - 32 * (p % 4), 1) if p % 4 else tile
        if r in (0, 7):
            ref = first if r == 0 else last
            for p in range(8):
                ref[2 * p] = main[r, p, :, :128]
                ref[2 * p + 1] = main[r, p, :, 128:]
            ref[16] = rows[:, :128]
            ref[17] = rows[:, 128:]


def field_slabs(main, ends, r):
    return [side(main[r, p], ends[r, p]) for p in range(8)]


def conv_rows(xs, w, bias, row, q, group=1):
    rhs = side(*[window(xs, row, 2 * q + s, group + 2, 3) for s in range(2)])
    res = dot(w, rhs)
    size = bias.shape[0]
    return {
        (r, s): silu(res[r * size : (r + 1) * size, s * WIDE : (s + 1) * WIDE] + bias)
        for r in range(group)
        for s in range(2)
    }


def inner_kernel(main, ends, w, b, skip, pooled, xs):
    flags = edges()
    for r in range(8):
        fill(xs, r, field_slabs(main, ends, r))
    mask = lane_mask(flags)
    bias = b[...]

    def one(k, carry):
        for q in range(4):
            for (r, s), y in conv_rows(xs, w[...], bias, 3 * k, q, 3).items():
                skip[3 * k + r, 2 * q + s] = (y * mask).astype(BF16)
        return carry

    lax.fori_loop(0, 2, one, 0)
    for k in range(2):
        for q in range(4):
            pooled[k, q] = mean([skip[2 * k + 1 + r, 2 * q + s] for r in range(2) for s in range(2)])


def mean(slabs):
    total = slabs[0].astype(F32)
    for slab in slabs[1:]:
        total = total + slab.astype(F32)
    return (total * 0.25).astype(BF16)


def outer_kernel(
    main, ends, above, below, skip_in, pooled_in, w, b, skip, pooled, p_first, p_last, xs
):
    flags = edges()
    fill(xs, 0, [unpack(above, p, 8) for p in range(8)], flags[0])
    for n, r in enumerate((0, 1)):
        fill(xs, 1 + n, field_slabs(main, ends, r))
    for n, r in enumerate((6, 7)):
        fill(xs, 3 + n, field_slabs(main, ends, r))
    fill(xs, 5, [unpack(below, p, 8) for p in range(8)], flags[1])
    mask = lane_mask(flags)
    bias = b[...]

    def one(k, carry):
        for q in range(4):
            for (r, s), y in conv_rows(xs, w[...], bias, 3 * k, q).items():
                skip[k, 2 * q + s] = (y * mask).astype(BF16)
        return carry

    lax.fori_loop(0, 2, one, 0)
    for q in range(4):
        pooled[0, q] = mean([src[0, 2 * q + s] for src in (skip, skip_in) for s in range(2)])
        far = [skip_in[5, 2 * q + s] for s in range(2)] + [skip[1, 2 * q + s] for s in range(2)]
        pooled[1, q] = mean(far)
    rows = [[ref[k, q] for q in range(4)] for ref, k in ((pooled, 0), (pooled_in, 0), (pooled_in, 1), (pooled, 1))]
    pack(p_first, rows[0] + rows[1] + rows[2])
    pack(p_last, rows[1] + rows[2] + rows[3])


def two_kernel(pooled_in, pooled, above, below, w2, b2, skip2, pooled2, first, last, xs):
    flags = edges()
    for r in range(3):
        fill(xs, r, [unpack(above, 4 * r + p, 12) for p in range(4)], flags[0])
        fill(xs, r + 7, [unpack(below, 4 * r + p, 12) for p in range(4)], flags[1])
    for n, (ref, r) in enumerate(((pooled, 0), (pooled_in, 0), (pooled_in, 1), (pooled, 1))):
        fill(xs, n + 3, [ref[r, p] for p in range(4)])
    mask = lane_mask(flags)
    bias = b2[...]

    def pair(k, carry):
        valid = jnp.where(k == 0, flags[0], jnp.where(k == 3, flags[1], 1.0))
        inside = mask * valid
        for q in range(2):
            slabs = []
            for (r, s), y in conv_rows(xs, w2[...], bias, 2 * k, q, 2).items():
                y = (y * inside).astype(BF16)
                skip2[2 * k + r, 2 * q + s] = y
                slabs.append(y)
            pooled2[k, q] = mean(slabs)
        return carry

    lax.fori_loop(0, 4, pair, 0)
    pack(first, [pooled2[r, p] for r in (2, 3) for p in range(2)])
    pack(last, [pooled2[r, p] for r in (0, 1) for p in range(2)])


def three_kernel(pooled2, above, below, w3, b3, wc, bc, skip3, coarse, send, xs, xc):
    flags = edges()
    for r in range(2):
        fill(xs, r, [unpack(above, 2 * r + p, 4) for p in range(2)], flags[0])
        fill(xs, r + 6, [unpack(below, 2 * r + p, 4) for p in range(2)], flags[1])
    for r in range(4):
        fill(xs, r + 2, [pooled2[r, p] for p in range(2)])
    mask = lane_mask(flags)
    for k in range(3):
        inside = mask * (flags[0] if k == 0 else flags[1]) if k != 1 else mask
        slabs = []
        for r in range(2):
            for (_, p), y in conv_rows(xs, w3[...], b3[...], 2 * k + r, 0).items():
                y = (y * inside).astype(BF16)
                skip3[2 * k + r, p] = y
                slabs.append(y)
        fill(xc, k, [mean(slabs)])
    res = silu(dot(wc[...], window(xc, 0, 0, 3, 3)) + bc[...])
    res = (res * mask).astype(BF16)
    coarse[...] = res
    size = res.shape[0] // 4
    pack(send, [res[n * size : (n + 1) * size] for n in range(4)])


def skip_three_kernel(s3, w, b, out, xs):
    for r in range(6):
        fill(xs, r, [s3[r, p] for p in range(2)])
    for r in range(4):
        res = dot(w[...], side(*[window(xs, r, p, 3, 3) for p in range(2)]))
        for p in range(2):
            out[r, p] = res[:, p * WIDE : (p + 1) * WIDE] + b[...]


def skip_two_kernel(s2, s_out, w, b, out, first, last, xs):
    for r in range(8):
        fill(xs, r, [s2[r, p] for p in range(4)])
    bias = b[...]

    def pair(k, carry):
        for q in range(2):
            res = dot(w[...], side(*[window(xs, 2 * k, 2 * q + s, 4, 3) for s in range(2)]))
            for r in range(2):
                for s in range(2):
                    part = res[r * bias.shape[0] : (r + 1) * bias.shape[0]]
                    out[2 * k + r, 2 * q + s] = part[:, s * WIDE : (s + 1) * WIDE] + bias
        return carry

    lax.fori_loop(0, 3, pair, 0)
    pack(first, [s_out[0, p] for p in range(8)])
    pack(last, [s_out[1, p] for p in range(8)])


def skip_inner_kernel(s_in, s_out, w, b, out, xs):
    fill(xs, 0, [s_out[0, p] for p in range(8)])
    for r in range(6):
        fill(xs, r + 1, [s_in[r, p] for p in range(8)])
    fill(xs, 7, [s_out[1, p] for p in range(8)])
    size = b.shape[0]
    for k in range(2):
        for p in range(8):
            res = dot(w[...], window(xs, 3 * k, p, 5, 3)[:, :256])
            for r in range(3):
                out[3 * k + r, p] = res[r * size : (r + 1) * size] + b[...]


def skip_outer_kernel(s_in, s_out, above, below, w, b, out, xs):
    flags = edges()
    fill(xs, 0, [unpack(above, p, 8) for p in range(8)], flags[0])
    for n, (ref, r) in enumerate(((s_out, 0), (s_in, 0), (s_in, 5), (s_out, 1))):
        fill(xs, n + 1, [ref[r, p] for p in range(8)])
    fill(xs, 5, [unpack(below, p, 8) for p in range(8)], flags[1])
    for k in range(2):
        for p in range(8):
            out[k, p] = dot(w[...], window(xs, 3 * k, p, 3, 3)[:, :256]) + b[...]


def back_kernel(c, above, below, pre3, pre2, wu3, wu2, out, xc, xb):
    flags = edges()
    halo = lambda packed: [jnp.concatenate([unpack(packed, n, 4) for n in range(4)], axis=0)]
    fill(xc, 0, halo(above), flags[0])
    fill(xc, 1, [c[...]])
    fill(xc, 2, halo(below), flags[1])
    mask = lane_mask(flags)
    slabs = {}
    for a in range(2):
        for p in range(2):
            res = dot(wu3[a, p], side(window(xc, 0, p, 2, 2), window(xc, 1, p, 2, 2)))
            for n in range(2):
                r = 2 * n + 1 - a
                y = silu(res[:, n * WIDE : (n + 1) * WIDE] + pre3[r, p])
                inside = mask * flags[0] if r == 0 else mask * flags[1] if r == 3 else mask
                slabs[r, p] = (y * inside).astype(BF16)
    for r in range(4):
        fill(xb, r, [slabs[r, p] for p in range(2)])

    def pair(k, carry):
        for b in range(2):
            rhs = side(*[window(xb, k, (p + 1) // 2, 2, 2) for p in (b, b + 2)])
            res = dot(wu2[b], rhs)
            size = res.shape[0] // 2
            for i in range(2):
                valid = jnp.where(
                    (k == 0) & (i == 0), flags[0], jnp.where((k == 2) & (i == 1), flags[1], 1.0)
                )
                inside = mask * valid
                rows = res[i * size : (i + 1) * size]
                for n in range(2):
                    y = silu(rows[:, n * WIDE : (n + 1) * WIDE] + pre2[2 * k + i, b + 2 * n])
                    out[2 * k + i, b + 2 * n] = (y * inside).astype(BF16)
        return carry

    lax.fori_loop(0, 3, pair, 0)


def last_kernel(bt, pre_in, pre_out, wu, out, xb):
    for r in range(6):
        fill(xb, r, [bt[r, p] for p in range(4)])
    size = wu.shape[0] // 4
    for k in range(5):
        for m in range(5):
            res = dot(wu[...], window(xb, k, m, 2, 2)[:, :256])
            for i in range(2):
                for j in range(2):
                    r, p = 2 * k - 1 + i, 2 * m - 1 + j
                    if not (0 <= r < 8 and 0 <= p < 8):
                        continue
                    pre = pre_out[0, p] if r == 0 else pre_out[1, p] if r == 7 else pre_in[r - 1, p]
                    n = 2 * (1 - i) + 1 - j
                    y = silu(res[n * size : (n + 1) * size] + pre).astype(BF16)
                    for h in range(2):
                        lanes = slice(h * 128, (h + 1) * 128)
                        out[h, r, :, p * 128 : (p + 1) * 128] = y[:, lanes]


def head_kernel_body(back, fields, w, offset, out, buf, sems):
    lane = iota((1, LANES), 1)
    c = iota((1, 256), 1)
    merge = one_hot(iota((256, 256), 0) == 32 * (c & 7) + (c >> 3))
    copies = []
    for h in range(2):
        for half in range(2):
            blocks = []
            for q in (2 * half, 2 * half + 1):
                pieces = []
                for g in range(2):
                    tile = rolled(back[h, :, g * 512 : g * 512 + 128], -32 * q)
                    for n in range(1, 4):
                        start = g * 512 + n * 128
                        piece = rolled(back[h, :, start : start + 128], 32 * (n - q))
                        tile = jnp.where(lane < 32 * n, tile, piece)
                    pieces.append(tile)
                blocks.append(dot(side(*pieces), merge).astype(BF16))
            cols = slice(half * 512, (half + 1) * 512)
            base = fields[h, :, cols].astype(F32) + side(offset[...], offset[...])
            buf[h, :, cols] = base + dot(w[...], side(*blocks))
            n = 2 * h + half
            copies.append(pltpu.make_async_copy(buf.at[h, :, cols], out.at[h, :, cols], sems.at[n]))
            copies[n].start()
    for copy in copies:
        copy.wait()


def flip(value):
    eye = one_hot(iota((value.shape[1],) * 2, 0) == iota((value.shape[1],) * 2, 1))
    dims = (((1,), (1,)), ((), ()))
    return lax.dot_general(eye, value, dims, preferred_element_type=F32).astype(BF16)


def column(row, width, repeat=1):
    size = row.shape[1]
    i, j = iota((size * repeat, size), 0), iota((size * repeat, size), 1)
    col = jnp.sum(jnp.where(i // repeat == j, row, 0.0), axis=1, keepdims=True)
    return jnp.broadcast_to(col, (size * repeat, width))


def sums(a):
    return ((0,), (1, 2)) if a == 0 else ((0, 1), (2,))


def summed(tap, a, b, i, j):
    total = None
    for dy in sums(a)[i]:
        for dx in sums(b)[j]:
            value = tap(dy, dx).astype(F32)
            total = value if total is None else total + value
    return total.astype(BF16)


def placed(parts, width):
    size = parts[0].shape[1]
    total = None
    for n, part in enumerate(parts):
        spot = one_hot(iota((size, width), 1) == iota((size, width), 0) + n * size)
        value = dot(part, spot)
        total = value if total is None else total + value
    return total.astype(BF16)


def grouped(w, rows):
    size, step = w.shape[1], w.shape[1] // 3
    width = step * (rows + 2)
    i, j = iota((size, width), 0), iota((size, width), 1)
    parts = [dot(w, one_hot(j == i + n * step)).astype(BF16) for n in range(rows)]
    return jnp.concatenate(parts, axis=0)


NINE = [(dy, dx) for dy in range(3) for dx in range(3)]
FOUR = [(i, j) for i in range(2) for j in range(2)]


def early_kernel(k1, k2, k3, r1, r2, r3, w1, g1, w2, w3, b1, b2, b3):
    w1[...] = placed([k1[n] for n in NINE], w1.shape[1])
    g1[...] = grouped(w1[...], 3)
    w2[...] = grouped(flip(k2[...].reshape(-1, k2.shape[3])), 2)
    w3[...] = flip(k3[...].reshape(-1, k3.shape[3]))
    for r, b in ((r1, b1), (r2, b2), (r3, b3)):
        b[...] = column(r[...], WIDE)


def late_kernel(
    kc, d3, d2, d1, hk, rc, r3, r2, r1, rh, wc, wu3, ws3, wu2, gs2, wu1, ws1, gs1, wh, bc, b3, b2, b1, bh
):
    wc[...] = flip(kc[...].reshape(-1, kc.shape[3]))
    for r, b in ((rc, bc), (r3, b3), (r2, b2), (r1, b1)):
        b[...] = column(r[...], b.shape[1])
    bh[...] = column(rh[...], bh.shape[1], 8)
    up3, up2, up1 = wu3.shape[3] // 4, wu2.shape[2] // 4, wu1.shape[1] // 4
    n2, n1 = d2.shape[2], d1.shape[2]
    for a in range(2):
        for b in range(2):
            tall = [summed(lambda y, x: d3[y, x, :up3, :], a, b, i, j) for i, j in FOUR]
            wu3[a, b] = flip(jnp.concatenate(tall, axis=0))
            wide = [summed(lambda y, x: d2[y, x, :, :up2], a, b, i, j) for i, j in FOUR]
            wu2[b, (1 - a) * n2 : (2 - a) * n2] = jnp.concatenate(wide, axis=1)
            wide = [summed(lambda y, x: d1[y, x, :, :up1], a, b, i, j) for i, j in FOUR]
            wu1[(2 * a + b) * n1 : (2 * a + b + 1) * n1] = placed(wide, wu1.shape[1])
    ws3[...] = flip(jnp.concatenate([d3[y, x, up3:, :] for y, x in NINE], axis=0))
    skips = [d2[y, x, :, up2:] for y, x in NINE]
    gs2[...] = grouped(placed(skips, 9 * skips[0].shape[1]), 2)
    ws1[...] = placed([d1[y, x, :, up1:] for y, x in NINE], ws1.shape[1])
    gs1[...] = grouped(ws1[...], 3)
    v, c = hk.shape[1], hk.shape[0]
    spread = one_hot(iota((v * 8, v), 0) // 8 == iota((v * 8, v), 1))
    dims = (((1,), (1,)), ((), ()))
    tall = lax.dot_general(spread, hk[...], dims, preferred_element_type=F32).astype(BF16)
    i, k = iota((v * 8, 8 * c), 0), iota((v * 8, 8 * c), 1)
    tiled = dot(tall, one_hot(iota((c, 8 * c), 0) == iota((c, 8 * c), 1) % c))
    wh[...] = jnp.where(i % 8 == k // c, tiled, 0.0).astype(BF16)


def body(
    fields,
    kernel_one,
    bias_one,
    kernel_two,
    bias_two,
    kernel_three,
    bias_three,
    kernel_coarse,
    bias_coarse,
    decode_three,
    offset_three,
    decode_two,
    offset_two,
    decode_one,
    offset_one,
    head_kernel,
    head_offset,
):
    c1, c2, c3, c4 = (k.shape[3] for k in (kernel_one, kernel_two, kernel_three, kernel_coarse))
    v = fields.shape[1]

    x = fields.reshape(2, v * 8, 1024)
    from_l = neighbour(x[:, :, 896:], "tx", 1)
    from_r = neighbour(x[:, :, :128], "tx", -1)

    def up(value):
        return neighbour(value, "ty", -1)

    def down(value):
        return neighbour(value, "ty", 1)

    row = lambda bias: bias[None, :]
    swap = lambda kernel: jnp.transpose(kernel, (0, 1, 3, 2))
    weights = lambda *shape: (shape, BF16)
    biases = lambda size, width=WIDE: ((size, width), F32)
    w1, g1, w2, w3, b1, b2, b3 = call(
        early_kernel,
        "early",
        [weights(c1, 9 * v), weights(3 * c1, 15 * v), weights(2 * c2, 12 * c1), weights(c3, 9 * c2)]
        + [biases(c1), biases(c2), biases(c3)],
        [],
        [swap(kernel_one), kernel_two, kernel_three, row(bias_one), row(bias_two), row(bias_three)],
    )
    wc, wu3, ws3, wu2, gs2, wu1, ws1, gs1, wh, bc, ob3, ob2, ob1, bh = call(
        late_kernel,
        "late",
        [weights(c4, 9 * c3), weights(2, 2, c3, 4 * c4), weights(c3, 9 * c3)]
        + [weights(2, 2 * c2, 4 * c3), weights(2 * c2, 12 * c2)]
        + [weights(4 * c1, 4 * c2), weights(c1, 9 * c1), weights(3 * c1, 15 * c1)]
        + [weights(8 * v, 8 * c1)]
        + [biases(c4), biases(c3), biases(c2), biases(c1, 256), biases(8 * v, 256)],
        [],
        [kernel_coarse, decode_three, swap(decode_two), swap(decode_one), head_kernel]
        + [row(b) for b in (bias_coarse, offset_three, offset_two, offset_one, head_offset)],
        flops=5 * 10**8,
    )
    (main,) = call(main_kernel, "main", [((8, 8, v, 256), BF16)], [], [x], flops=10**9)
    packed = lambda count, size: ((tiles(count), size, LANES), BF16)
    ends, f_first, f_last = call(
        ends_kernel,
        "ends",
        [((8, 8, v, LANES), BF16), packed(8, v), packed(8, v)],
        [],
        [x, main, from_l, from_r],
    )
    f_above, f_below = down(f_last), up(f_first)
    s_in, p_in = call(
        inner_kernel,
        "inner",
        [((6, 8, c1, WIDE), BF16), ((2, 4, c1, WIDE), BF16)],
        [pltpu.VMEM((8, 10, v, WIDE), BF16)],
        [main, ends, g1, b1],
        flops=10**9,
    )
    s_out, p_out, p_first, p_last = call(
        outer_kernel,
        "outer",
        [((2, 8, c1, WIDE), BF16), ((2, 4, c1, WIDE), BF16)]
        + [packed(12, c1)] * 2,
        [pltpu.VMEM((6, 10, v, WIDE), BF16)],
        [main, ends, f_above, f_below, s_in, p_in, w1, b1],
    )
    p_above, p_below = down(p_last), up(p_first)
    s2, p2, q_first, q_last = call(
        two_kernel,
        "two",
        [((8, 4, c2, WIDE), BF16), ((4, 2, c2, WIDE), BF16), packed(4, c2), packed(4, c2)],
        [pltpu.VMEM((10, 6, c1, WIDE), BF16)],
        [p_in, p_out, p_above, p_below, w2, b2],
    )
    q_above, q_below = down(q_last), up(q_first)
    pre2, s_first, s_last = call(
        skip_two_kernel,
        "skip_two",
        [((6, 4, c2, WIDE), F32), packed(8, c1), packed(8, c1)],
        [pltpu.VMEM((8, 6, c2, WIDE), BF16)],
        [s2, s_out, gs2, ob2],
        flops=10**9,
    )
    s_above, s_below = down(s_last), up(s_first)
    s3, coarse, c_send = call(
        three_kernel,
        "three",
        [((6, 2, c3, WIDE), BF16), ((c4, WIDE), BF16), packed(4, c4 // 4)],
        [pltpu.VMEM((8, 4, c2, WIDE), BF16), pltpu.VMEM((3, 3, c3, WIDE), BF16)],
        [p2, q_above, q_below, w3, b3, wc, bc],
    )
    c_above, c_below = down(c_send), up(c_send)
    (pre_in,) = call(
        skip_inner_kernel,
        "skip_inner",
        [((6, 8, c1, 256), F32)],
        [pltpu.VMEM((8, 10, c1, WIDE), BF16)],
        [s_in, s_out, gs1, ob1],
        flops=10**9,
    )
    (pre_out,) = call(
        skip_outer_kernel,
        "skip_outer",
        [((2, 8, c1, 256), F32)],
        [pltpu.VMEM((6, 10, c1, WIDE), BF16)],
        [s_in, s_out, s_above, s_below, ws1, ob1],
        flops=5 * 10**8,
    )
    (pre3,) = call(
        skip_three_kernel,
        "skip_three",
        [((4, 2, c3, WIDE), F32)],
        [pltpu.VMEM((6, 4, c3, WIDE), BF16)],
        [s3, ws3, ob3],
        flops=10**9,
    )
    (back_two,) = call(
        back_kernel,
        "back",
        [((6, 4, c2, WIDE), BF16)],
        [pltpu.VMEM((3, 3, c4, WIDE), BF16), pltpu.VMEM((4, 4, c3, WIDE), BF16)],
        [coarse, c_above, c_below, pre3, pre2, wu3, wu2],
    )
    (back_one,) = call(
        last_kernel,
        "last",
        [((2, 8, c1, 1024), BF16)],
        [pltpu.VMEM((6, 6, c2, WIDE), BF16)],
        [back_two, pre_in, pre_out, wu1],
    )
    out = pl.pallas_call(
        head_kernel_body,
        name="head",
        out_shape=jax.ShapeDtypeStruct((2, v * 8, 1024), F32),
        in_specs=[pl.BlockSpec(memory_space=pltpu.VMEM)] * 4,
        out_specs=pl.BlockSpec(memory_space=pl.ANY),
        scratch_shapes=[pltpu.VMEM((2, v * 8, 1024), F32), pltpu.SemaphoreType.DMA((4,))],
        compiler_params=pltpu.CompilerParams(vmem_limit_bytes=16 * 2**20),
    )(back_one.reshape(2, 8 * c1, 1024), x, wh, bh)
    return out.reshape(2, v, 8, 1024)


def solution(mesh):
    return jax.shard_map(
        body,
        mesh=mesh,
        in_specs=(P(None, None, "ty", "tx"),) + (P(),) * 16,
        out_specs=P(None, None, "ty", "tx"),
        check_vma=False,
    )
```

```python
import jax
import jax.numpy as jnp
from jax import lax
from jax.experimental import pallas as pl
from jax.experimental.pallas import tpu as pltpu
from jax.sharding import PartitionSpec as P

LANES = 128
WIDE = 384
BF16 = jnp.bfloat16
F32 = jnp.float32


def swap(near_part, far_part, axis):
    size = lax.axis_size(axis)
    near = [(i, i ^ 1) for i in range(size)]
    far = [(i, (i + 1 if i % 2 else i - 1) % size) for i in range(size)]
    return lax.ppermute(near_part, axis, near), lax.ppermute(far_part, axis, far)


class Either:
    def __init__(self, cond, one, other):
        self.cond, self.one, self.other = cond, one, other

    def __getitem__(self, index):
        return jnp.where(self.cond, self.one[index], self.other[index])


def is_even(axis):
    return lax.axis_index(axis) % 2 == 0


def received(near, far, axis):
    even = is_even(axis)
    return Either(even, far, near), Either(even, near, far)


def pack_both(near, far, before, after):
    even = is_even("ty")
    pack(near, [jnp.where(even, b, a) for a, b in zip(before, after)])
    pack(far, [jnp.where(even, a, b) for a, b in zip(before, after)])


def call(body, name, out_shapes, scratch, args, limit=16, flops=0):
    specs = [pl.BlockSpec(memory_space=pltpu.VMEM)] * len(args)
    return pl.pallas_call(
        body,
        name=name,
        out_shape=[jax.ShapeDtypeStruct(s, d) for s, d in out_shapes],
        in_specs=specs,
        out_specs=[pl.BlockSpec(memory_space=pltpu.VMEM)] * len(out_shapes),
        scratch_shapes=scratch,
        cost_estimate=pl.CostEstimate(flops=flops, transcendentals=0, bytes_accessed=0),
        compiler_params=pltpu.CompilerParams(vmem_limit_bytes=limit * 2**20),
    )(*args)


def iota(shape, axis):
    return lax.broadcasted_iota(jnp.int32, shape, axis)


def edges():
    ty, tx = lax.axis_index("ty"), lax.axis_index("tx")
    ny, nx = lax.axis_size("ty"), lax.axis_size("tx")
    inside = (ty > 0, ty < ny - 1, tx > 0, tx < nx - 1)
    return [jnp.where(side, 1.0, 0.0) for side in inside]


def one_hot(cond):
    return jnp.where(cond, 1.0, 0.0).astype(BF16)


def dot(a, b):
    return jnp.dot(a, b, preferred_element_type=F32)


def silu(t):
    return t * (0.5 * jnp.tanh(0.5 * t) + 0.5)


def lane_mask(flags):
    lane = iota((1, WIDE), 1)
    place = lane & 15
    edge = lane >= 256
    left = jnp.where(edge & (place < 4), flags[2], 1.0)
    right = jnp.where(edge & (place >= 12), flags[3], 1.0)
    return left * right


def from_left(slab):
    lane = iota((1, LANES), 1)
    h0, h1, edge = slab[:, :128], slab[:, 128:256], slab[:, 256:]
    h0 = jnp.where(lane == 0, pltpu.roll(edge, 125, 1), pltpu.roll(h0, 1, 1))
    h1 = jnp.where(lane == 0, pltpu.roll(edge, 109, 1), pltpu.roll(h1, 1, 1))
    return jnp.concatenate([h0, h1, pltpu.roll(edge, 1, 1)], axis=1)


def from_right(slab):
    lane = iota((1, LANES), 1)
    h0, h1, edge = slab[:, :128], slab[:, 128:256], slab[:, 256:]
    h0 = jnp.where(lane == 127, pltpu.roll(edge, 115, 1), pltpu.roll(h0, 127, 1))
    h1 = jnp.where(lane == 127, pltpu.roll(edge, 99, 1), pltpu.roll(h1, 127, 1))
    return jnp.concatenate([h0, h1, pltpu.roll(edge, 127, 1)], axis=1)


def fill(scratch, row, slabs, valid=None):
    phases = len(slabs)
    for p, slab in enumerate(slabs):
        if valid is not None:
            slab = jnp.where(valid > 0.5, slab, jnp.zeros_like(slab))
        scratch[row, p + 1] = slab
        if p == 0:
            scratch[row, phases + 1] = from_right(slab)
        if p == phases - 1:
            scratch[row, 0] = from_left(slab)


def window(scratch, row, phase, rows, cols):
    v = scratch[pl.ds(row, rows), phase : phase + cols]
    return v.reshape(rows * cols * v.shape[2], v.shape[3])


def side(*parts):
    return jnp.concatenate(parts, axis=1)


def pack(out, slabs):
    lane = iota((1, LANES), 1)
    count = len(slabs)
    for n, slab in enumerate(slabs):
        out[2 * n] = slab[:, :128]
        out[2 * n + 1] = slab[:, 128:256]
    for g in range(0, count, 4):
        tile = slabs[g][:, 256:]
        for n in range(1, min(4, count - g)):
            tile = jnp.where(lane < 32 * n, tile, pltpu.roll(slabs[g + n][:, 256:], 32 * n, 1))
        out[2 * count + g // 4] = tile


def unpack(packed, n, count):
    tile = packed[2 * count + n // 4]
    if n % 4:
        tile = pltpu.roll(tile, 128 - 32 * (n % 4), 1)
    return side(packed[2 * n], packed[2 * n + 1], tile)


def tiles(count):
    return 2 * count + (count + 3) // 4


def turned(part):
    rows = part.shape[0]
    i, k = iota((rows, rows), 0), iota((rows, rows), 1)
    turn = one_hot(i == (k & 7) * (rows // 8) + (k >> 3))
    return dot(turn, part).astype(BF16)


def cols_kernel(x, near, far):
    lane = iota((1, LANES), 1)
    size = x.shape[1] // 4
    even = is_even("tx")
    for h in range(2):
        packed = []
        for start, first in ((0, 0), (896, 96)):
            tile = None
            for g in range(4):
                rows = slice(g * size, (g + 1) * size)
                piece = rolled(x[h, rows, start : start + 128], 32 * g - first)
                tile = piece if tile is None else jnp.where(lane < 32 * g, tile, piece)
            packed.append(tile)
        near[h] = jnp.where(even, packed[1], packed[0])
        far[h] = jnp.where(even, packed[0], packed[1])


def columns(packed, first):
    return jnp.concatenate([rolled(packed, first - 32 * g) for g in range(4)], axis=0)


def main_kernel(x, out):
    channels = x.shape[1] // 8
    lane = iota((1, LANES), 1)
    c = iota((1, 256), 1)
    split = one_hot(iota((256, 256), 0) == 8 * (c & 31) + (c >> 5))
    for h in range(2):
        blocks = [dot(x[h, :, q * 256 : (q + 1) * 256], split).astype(BF16) for q in range(4)]
        phases = []
        for p in range(8):
            half = slice((p // 4) * 128, (p // 4 + 1) * 128)
            tile = rolled(blocks[0][:, half], -32 * (p % 4))
            for q in range(1, 4):
                tile = jnp.where(lane < 32 * q, tile, rolled(blocks[q][:, half], 32 * (q - p % 4)))
            phases.append(tile)
        for q in range(4):
            part = turned(side(phases[2 * q], phases[2 * q + 1]))
            for r in range(8):
                rows = part[r * channels : (r + 1) * channels]
                for s in range(2):
                    out[r, 2 * q + s, :, h * 128 : (h + 1) * 128] = rows[:, s * 128 : (s + 1) * 128]


def rolled(value, shift):
    return pltpu.roll(value, shift % 128, 1) if shift % 128 else value


def ends_kernel(x, main, cols_near, cols_far, out, near, far):
    flags = edges()
    fl, fr = received(cols_near, cols_far, "tx")
    lane = iota((1, LANES), 1)
    channels = x.shape[1] // 8
    ends = []
    for h in range(2):
        before, after = columns(fl[h], 96), columns(fr[h], 0)
        a = jnp.where((lane >= 96) & (flags[2] > 0.5), before, jnp.where(lane < 32, x[h, :, :128], 0))
        b = jnp.where(lane >= 96, x[h, :, 896:], jnp.where((lane < 32) & (flags[3] > 0.5), after, 0))
        ends += [a.astype(BF16), b.astype(BF16)]
    ends = side(*ends)
    c = iota((1, 256), 1)
    row = 128 * ((c & 31) >> 3) + (((8 * (c & 7) + (c >> 5)) + 96) & 127)
    part = turned(dot(ends, one_hot(iota((512, 256), 0) == row)).astype(BF16))
    for r in range(8):
        rows = part[r * channels : (r + 1) * channels]
        for p in range(8):
            tile = rows[:, (p // 4) * 128 : (p // 4 + 1) * 128]
            out[r, p] = pltpu.roll(tile, 128 - 32 * (p % 4), 1) if p % 4 else tile
    pack_both(near, far, field_slabs(main, out, 0), field_slabs(main, out, 7))


def field_slabs(main, ends, r):
    return [side(main[r, p], ends[r, p]) for p in range(8)]


def conv_rows(xs, w, bias, row, q, group=1):
    rhs = side(*[window(xs, row, 2 * q + s, group + 2, 3) for s in range(2)])
    res = dot(w, rhs)
    size = bias.shape[0]
    return {
        (r, s): silu(res[r * size : (r + 1) * size, s * WIDE : (s + 1) * WIDE] + bias)
        for r in range(group)
        for s in range(2)
    }


def inner_kernel(main, ends, w, w_low, w_high, b, skip, pooled, outer, xs):
    flags = edges()
    for r in range(8):
        fill(xs, r, field_slabs(main, ends, r))
    mask = lane_mask(flags)
    bias = b[...]

    def one(k, carry):
        for q in range(4):
            for (r, s), y in conv_rows(xs, w[...], bias, 3 * k, q, 3).items():
                skip[3 * k + r, 2 * q + s] = (y * mask).astype(BF16)
        return carry

    lax.fori_loop(0, 2, one, 0)
    for k, (row, part) in enumerate(((0, w_low), (6, w_high))):
        for q in range(4):
            res = dot(part[...], side(*[window(xs, row, 2 * q + s, 2, 3) for s in range(2)]))
            for s in range(2):
                outer[k, 2 * q + s] = res[:, s * WIDE : (s + 1) * WIDE] + bias
    for k in range(2):
        for q in range(4):
            pooled[k, q] = mean([skip[2 * k + 1 + r, 2 * q + s] for r in range(2) for s in range(2)])


def mean(slabs):
    total = slabs[0].astype(F32)
    for slab in slabs[1:]:
        total = total + slab.astype(F32)
    return (total * 0.25).astype(BF16)


def outer_kernel(
    f_near, f_far, partial, skip_in, pooled_in, w_top, w_bottom, skip, pooled, near, far, xs
):
    flags = edges()
    above, below = received(f_near, f_far, "ty")
    fill(xs, 0, [unpack(above, p, 8) for p in range(8)], flags[0])
    fill(xs, 1, [unpack(below, p, 8) for p in range(8)], flags[1])
    mask = lane_mask(flags)
    for k, part in enumerate((w_top, w_bottom)):
        for q in range(4):
            res = dot(part[...], side(*[window(xs, k, 2 * q + s, 1, 3) for s in range(2)]))
            for s in range(2):
                y = silu(res[:, s * WIDE : (s + 1) * WIDE] + partial[k, 2 * q + s])
                skip[k, 2 * q + s] = (y * mask).astype(BF16)
    for q in range(4):
        pooled[0, q] = mean([src[0, 2 * q + s] for src in (skip, skip_in) for s in range(2)])
        ends = [skip_in[5, 2 * q + s] for s in range(2)] + [skip[1, 2 * q + s] for s in range(2)]
        pooled[1, q] = mean(ends)
    rows = [[ref[k, q] for q in range(4)] for ref, k in ((pooled, 0), (pooled_in, 0), (pooled_in, 1), (pooled, 1))]
    pack_both(near, far, rows[0] + rows[1] + rows[2], rows[1] + rows[2] + rows[3])


def middle_kernel(pooled_in, pooled, w2, b2, skip, xs):
    for n, (ref, r) in enumerate(((pooled, 0), (pooled_in, 0), (pooled_in, 1), (pooled, 1))):
        fill(xs, n, [ref[r, p] for p in range(4)])
    mask = lane_mask(edges())
    for q in range(2):
        for (r, s), y in conv_rows(xs, w2[...], b2[...], 0, q, 2).items():
            skip[r, 2 * q + s] = (y * mask).astype(BF16)


def two_kernel(pooled_in, pooled, p_near, p_far, middle, g2, b2, _, skip2, pooled2, near, far, xs):
    flags = edges()
    above, below = received(p_near, p_far, "ty")
    for r in range(3):
        fill(xs, r, [unpack(above, 4 * r + p, 12) for p in range(4)], flags[0])
        fill(xs, r + 5, [unpack(below, 4 * r + p, 12) for p in range(4)], flags[1])
    for n, (ref, r) in enumerate(((pooled, 0), (pooled_in, 0))):
        fill(xs, n + 3, [ref[r, p] for p in range(4)])
    for n, (ref, r) in enumerate(((pooled_in, 1), (pooled, 1))):
        fill(xs, n + 8, [ref[r, p] for p in range(4)])
    mask = lane_mask(flags)
    size = b2.shape[0]
    for k, first in ((0, 0), (1, 3)):
        rows = ((0, 1, 2, 3, 4), (8, 9, 5, 6, 7))[k]
        outside = mask * flags[k]
        for p in range(4):
            rhs = [window(xs, row, p, 1, 3) for row in rows]
            res = dot(g2[...], jnp.concatenate(rhs, axis=0))
            for r in range(3):
                inside = mask if r == (2, 0)[k] else outside
                y = silu(res[r * size : (r + 1) * size] + b2[...]) * inside
                skip2[first + r, p] = y.astype(BF16)
    order = [(skip2, 0), (skip2, 1), (skip2, 2), (middle, 0), (middle, 1), (skip2, 3), (skip2, 4), (skip2, 5)]
    for k in range(4):
        for q in range(2):
            pooled2[k, q] = mean([ref[r, 2 * q + s] for ref, r in order[2 * k : 2 * k + 2] for s in range(2)])
    before = [pooled2[r, p] for r in (2, 3) for p in range(2)]
    pack_both(near, far, before, [pooled2[r, p] for r in (0, 1) for p in range(2)])


def three_kernel(pooled2, q_near, q_far, w3, b3, wc, bc, skip3, coarse, send, xs, xc):
    flags = edges()
    above, below = received(q_near, q_far, "ty")
    for r in range(2):
        fill(xs, r, [unpack(above, 2 * r + p, 4) for p in range(2)], flags[0])
        fill(xs, r + 6, [unpack(below, 2 * r + p, 4) for p in range(2)], flags[1])
    for r in range(4):
        fill(xs, r + 2, [pooled2[r, p] for p in range(2)])
    mask = lane_mask(flags)
    for k in range(3):
        inside = mask * (flags[0] if k == 0 else flags[1]) if k != 1 else mask
        slabs = []
        for r in range(2):
            for (_, p), y in conv_rows(xs, w3[...], b3[...], 2 * k + r, 0).items():
                y = (y * inside).astype(BF16)
                skip3[2 * k + r, p] = y
                slabs.append(y)
        fill(xc, k, [mean(slabs)])
    res = silu(dot(wc[...], window(xc, 0, 0, 3, 3)) + bc[...])
    res = (res * mask).astype(BF16)
    coarse[...] = res
    size = res.shape[0] // 4
    pack(send, [res[n * size : (n + 1) * size] for n in range(4)])


def skip_three_kernel(s3, w, b, out, xs):
    for r in range(6):
        fill(xs, r, [s3[r, p] for p in range(2)])
    for r in range(4):
        res = dot(w[...], side(*[window(xs, r, p, 3, 3) for p in range(2)]))
        for p in range(2):
            out[r, p] = res[:, p * WIDE : (p + 1) * WIDE] + b[...]


def skip_two_kernel(s2, middle, s_out, w, b, out, near, far, xs):
    order = [(s2, 0), (s2, 1), (s2, 2), (middle, 0), (middle, 1), (s2, 3), (s2, 4), (s2, 5)]
    for n, (ref, r) in enumerate(order):
        fill(xs, n, [ref[r, p] for p in range(4)])
    bias = b[...]

    def pair(k, carry):
        for q in range(2):
            res = dot(w[...], side(*[window(xs, 2 * k, 2 * q + s, 4, 3) for s in range(2)]))
            for r in range(2):
                for s in range(2):
                    part = res[r * bias.shape[0] : (r + 1) * bias.shape[0]]
                    out[2 * k + r, 2 * q + s] = part[:, s * WIDE : (s + 1) * WIDE] + bias
        return carry

    lax.fori_loop(0, 3, pair, 0)
    pack_both(near, far, [s_out[0, p] for p in range(8)], [s_out[1, p] for p in range(8)])


def skip_inner_kernel(s_in, s_out, w, b, out, xs):
    fill(xs, 0, [s_out[0, p] for p in range(8)])
    for r in range(6):
        fill(xs, r + 1, [s_in[r, p] for p in range(8)])
    fill(xs, 7, [s_out[1, p] for p in range(8)])
    size = b.shape[0]
    for k in range(2):
        for p in range(8):
            res = dot(w[...], window(xs, 3 * k, p, 5, 3)[:, :256])
            for r in range(3):
                out[3 * k + r, p] = res[r * size : (r + 1) * size] + b[...]


def skip_outer_kernel(s_in, s_out, s_near, s_far, w, b, out, xs):
    flags = edges()
    above, below = received(s_near, s_far, "ty")
    fill(xs, 0, [unpack(above, p, 8) for p in range(8)], flags[0])
    for n, (ref, r) in enumerate(((s_out, 0), (s_in, 0), (s_in, 5), (s_out, 1))):
        fill(xs, n + 1, [ref[r, p] for p in range(8)])
    fill(xs, 5, [unpack(below, p, 8) for p in range(8)], flags[1])
    for k in range(2):
        for p in range(8):
            out[k, p] = dot(w[...], window(xs, 3 * k, p, 3, 3)[:, :256]) + b[...]


def back_kernel(c, c_near, c_far, pre3, pre2, wu3, wu2, out, xc, xb):
    flags = edges()
    above, below = received(c_near, c_far, "ty")
    halo = lambda packed: [jnp.concatenate([unpack(packed, n, 4) for n in range(4)], axis=0)]
    fill(xc, 0, halo(above), flags[0])
    fill(xc, 1, [c[...]])
    fill(xc, 2, halo(below), flags[1])
    mask = lane_mask(flags)
    slabs = {}
    for a in range(2):
        for p in range(2):
            res = dot(wu3[a, p], side(window(xc, 0, p, 2, 2), window(xc, 1, p, 2, 2)))
            for n in range(2):
                r = 2 * n + 1 - a
                y = silu(res[:, n * WIDE : (n + 1) * WIDE] + pre3[r, p])
                inside = mask * flags[0] if r == 0 else mask * flags[1] if r == 3 else mask
                slabs[r, p] = (y * inside).astype(BF16)
    for r in range(4):
        fill(xb, r, [slabs[r, p] for p in range(2)])

    def pair(k, carry):
        for b in range(2):
            rhs = side(*[window(xb, k, (p + 1) // 2, 2, 2) for p in (b, b + 2)])
            res = dot(wu2[b], rhs)
            size = res.shape[0] // 2
            for i in range(2):
                valid = jnp.where(
                    (k == 0) & (i == 0), flags[0], jnp.where((k == 2) & (i == 1), flags[1], 1.0)
                )
                inside = mask * valid
                rows = res[i * size : (i + 1) * size]
                for n in range(2):
                    y = silu(rows[:, n * WIDE : (n + 1) * WIDE] + pre2[2 * k + i, b + 2 * n])
                    out[2 * k + i, b + 2 * n] = (y * inside).astype(BF16)
        return carry

    lax.fori_loop(0, 3, pair, 0)


def last_kernel(bt, pre_in, pre_out, wu, out, xb):
    for r in range(6):
        fill(xb, r, [bt[r, p] for p in range(4)])
    size = wu.shape[0] // 4
    for k in range(5):
        for m in range(5):
            res = dot(wu[...], window(xb, k, m, 2, 2)[:, :256])
            for i in range(2):
                for j in range(2):
                    r, p = 2 * k - 1 + i, 2 * m - 1 + j
                    if not (0 <= r < 8 and 0 <= p < 8):
                        continue
                    pre = pre_out[0, p] if r == 0 else pre_out[1, p] if r == 7 else pre_in[r - 1, p]
                    n = 2 * (1 - i) + 1 - j
                    y = silu(res[n * size : (n + 1) * size] + pre).astype(BF16)
                    for h in range(2):
                        lanes = slice(h * 128, (h + 1) * 128)
                        out[h, r, :, p * 128 : (p + 1) * 128] = y[:, lanes]


def head_kernel_body(fields, back, w, offset, out, buf, sems):
    lane = iota((1, LANES), 1)
    c = iota((1, 256), 1)
    merge = one_hot(iota((256, 256), 0) == 32 * (c & 7) + (c >> 3))
    copies = []
    for h in range(2):
        for half in range(2):
            blocks = []
            for q in (2 * half, 2 * half + 1):
                pieces = []
                for g in range(2):
                    tile = rolled(back[h, :, g * 512 : g * 512 + 128], -32 * q)
                    for n in range(1, 4):
                        start = g * 512 + n * 128
                        piece = rolled(back[h, :, start : start + 128], 32 * (n - q))
                        tile = jnp.where(lane < 32 * n, tile, piece)
                    pieces.append(tile)
                blocks.append(dot(side(*pieces), merge).astype(BF16))
            cols = slice(half * 512, (half + 1) * 512)
            base = fields[h, :, cols].astype(F32) + side(offset[...], offset[...])
            buf[h, :, cols] = base + dot(w[...], side(*blocks))
            n = 2 * h + half
            copies.append(pltpu.make_async_copy(buf.at[h, :, cols], out.at[h, :, cols], sems.at[n]))
            copies[n].start()
    for copy in copies:
        copy.wait()


def flip(value):
    eye = one_hot(iota((value.shape[1],) * 2, 0) == iota((value.shape[1],) * 2, 1))
    dims = (((1,), (1,)), ((), ()))
    return lax.dot_general(eye, value, dims, preferred_element_type=F32).astype(BF16)


def column(row, width, repeat=1):
    size = row.shape[1]
    i, j = iota((size * repeat, size), 0), iota((size * repeat, size), 1)
    col = jnp.sum(jnp.where(i // repeat == j, row, 0.0), axis=1, keepdims=True)
    return jnp.broadcast_to(col, (size * repeat, width))


def sums(a):
    return ((0,), (1, 2)) if a == 0 else ((0, 1), (2,))


def summed(tap, a, b, i, j):
    total = None
    for dy in sums(a)[i]:
        for dx in sums(b)[j]:
            value = tap(dy, dx).astype(F32)
            total = value if total is None else total + value
    return total.astype(BF16)


def placed(parts, width):
    size = parts[0].shape[1]
    total = None
    for n, part in enumerate(parts):
        spot = one_hot(iota((size, width), 1) == iota((size, width), 0) + n * size)
        value = dot(part, spot)
        total = value if total is None else total + value
    return total.astype(BF16)


def grouped(w, rows):
    size, step = w.shape[1], w.shape[1] // 3
    width = step * (rows + 2)
    i, j = iota((size, width), 0), iota((size, width), 1)
    parts = [dot(w, one_hot(j == i + n * step)).astype(BF16) for n in range(rows)]
    return jnp.concatenate(parts, axis=0)


NINE = [(dy, dx) for dy in range(3) for dx in range(3)]
FOUR = [(i, j) for i in range(2) for j in range(2)]


def early_kernel(k1, k2, k3, r1, r2, r3, g1, low, high, top, bottom, w2, g2, w3, b1, b2, b3):
    w1 = placed([k1[n] for n in NINE], 9 * k1.shape[3])
    step = 3 * k1.shape[3]
    g1[...] = grouped(w1, 3)
    for ref, start in ((low, step), (high, 0), (top, 0), (bottom, 2 * step)):
        i, j = iota((w1.shape[1], ref.shape[1]), 0), iota((w1.shape[1], ref.shape[1]), 1)
        ref[...] = dot(w1, one_hot(i == j + start)).astype(BF16)
    flat = flip(k2[...].reshape(-1, k2.shape[3]))
    w2[...] = grouped(flat, 2)
    g2[...] = grouped(flat, 3)
    w3[...] = flip(k3[...].reshape(-1, k3.shape[3]))
    for r, b in ((r1, b1), (r2, b2), (r3, b3)):
        b[...] = column(r[...], WIDE)


def late_kernel(
    kc, d3, d2, d1, hk, rc, r3, r2, r1, rh, wc, wu3, ws3, wu2, gs2, wu1, ws1, gs1, wh, bc, b3, b2, b1, bh
):
    wc[...] = flip(kc[...].reshape(-1, kc.shape[3]))
    for r, b in ((rc, bc), (r3, b3), (r2, b2), (r1, b1)):
        b[...] = column(r[...], b.shape[1])
    bh[...] = column(rh[...], bh.shape[1], 8)
    up3, up2, up1 = wu3.shape[3] // 4, wu2.shape[2] // 4, wu1.shape[1] // 4
    n2, n1 = d2.shape[2], d1.shape[2]
    for a in range(2):
        for b in range(2):
            tall = [summed(lambda y, x: d3[y, x, :up3, :], a, b, i, j) for i, j in FOUR]
            wu3[a, b] = flip(jnp.concatenate(tall, axis=0))
            wide = [summed(lambda y, x: d2[y, x, :, :up2], a, b, i, j) for i, j in FOUR]
            wu2[b, (1 - a) * n2 : (2 - a) * n2] = jnp.concatenate(wide, axis=1)
            wide = [summed(lambda y, x: d1[y, x, :, :up1], a, b, i, j) for i, j in FOUR]
            wu1[(2 * a + b) * n1 : (2 * a + b + 1) * n1] = placed(wide, wu1.shape[1])
    ws3[...] = flip(jnp.concatenate([d3[y, x, up3:, :] for y, x in NINE], axis=0))
    skips = [d2[y, x, :, up2:] for y, x in NINE]
    gs2[...] = grouped(placed(skips, 9 * skips[0].shape[1]), 2)
    ws1[...] = placed([d1[y, x, :, up1:] for y, x in NINE], ws1.shape[1])
    gs1[...] = grouped(ws1[...], 3)
    v, c = hk.shape[1], hk.shape[0]
    spread = one_hot(iota((v * 8, v), 0) // 8 == iota((v * 8, v), 1))
    dims = (((1,), (1,)), ((), ()))
    tall = lax.dot_general(spread, hk[...], dims, preferred_element_type=F32).astype(BF16)
    i, k = iota((v * 8, 8 * c), 0), iota((v * 8, 8 * c), 1)
    tiled = dot(tall, one_hot(iota((c, 8 * c), 0) == iota((c, 8 * c), 1) % c))
    wh[...] = jnp.where(i % 8 == k // c, tiled, 0.0).astype(BF16)


def body(
    fields,
    kernel_one,
    bias_one,
    kernel_two,
    bias_two,
    kernel_three,
    bias_three,
    kernel_coarse,
    bias_coarse,
    decode_three,
    offset_three,
    decode_two,
    offset_two,
    decode_one,
    offset_one,
    head_kernel,
    head_offset,
):
    c1, c2, c3, c4 = (k.shape[3] for k in (kernel_one, kernel_two, kernel_three, kernel_coarse))
    v = fields.shape[1]

    x = fields.reshape(2, v * 8, 1024)
    near, far = call(cols_kernel, "cols", [((2, 2 * v, LANES), BF16)] * 2, [], [x])
    cols = swap(near, far, "tx")

    row = lambda bias: bias[None, :]
    turn = lambda kernel: jnp.transpose(kernel, (0, 1, 3, 2))
    weights = lambda *shape: (shape, BF16)
    biases = lambda size, width=WIDE: ((size, width), F32)
    g1, w_low, w_high, w_top, w_bottom, w2, g2, w3, b1, b2, b3 = call(
        early_kernel,
        "early",
        [weights(3 * c1, 15 * v)]
        + [weights(c1, rows * 3 * v) for rows in (2, 2, 1, 1)]
        + [weights(2 * c2, 12 * c1), weights(3 * c2, 15 * c1), weights(c3, 9 * c2)]
        + [biases(c1), biases(c2), biases(c3)],
        [],
        [turn(kernel_one), kernel_two, kernel_three, row(bias_one), row(bias_two), row(bias_three)],
    )
    wc, wu3, ws3, wu2, gs2, wu1, ws1, gs1, wh, bc, ob3, ob2, ob1, bh = call(
        late_kernel,
        "late",
        [weights(c4, 9 * c3), weights(2, 2, c3, 4 * c4), weights(c3, 9 * c3)]
        + [weights(2, 2 * c2, 4 * c3), weights(2 * c2, 12 * c2)]
        + [weights(4 * c1, 4 * c2), weights(c1, 9 * c1), weights(3 * c1, 15 * c1)]
        + [weights(8 * v, 8 * c1)]
        + [biases(c4), biases(c3), biases(c2), biases(c1, 256), biases(8 * v, 256)],
        [],
        [kernel_coarse, decode_three, turn(decode_two), turn(decode_one), head_kernel]
        + [row(b) for b in (bias_coarse, offset_three, offset_two, offset_one, head_offset)],
        flops=5 * 10**8,
    )
    (main,) = call(main_kernel, "main", [((8, 8, v, 256), BF16)], [], [x], flops=10**9)
    packed = lambda count, size: ((tiles(count), size, LANES), BF16)
    ends, near, far = call(
        ends_kernel,
        "ends",
        [((8, 8, v, LANES), BF16), packed(8, v), packed(8, v)],
        [],
        [x, main, *cols],
    )
    halo = swap(near, far, "ty")
    s_in, p_in, partial = call(
        inner_kernel,
        "inner",
        [((6, 8, c1, WIDE), BF16), ((2, 4, c1, WIDE), BF16), ((2, 8, c1, WIDE), F32)],
        [pltpu.VMEM((8, 10, v, WIDE), BF16)],
        [main, ends, g1, w_low, w_high, b1],
        flops=10**9,
    )
    s_out, p_out, near, far = call(
        outer_kernel,
        "outer",
        [((2, 8, c1, WIDE), BF16), ((2, 4, c1, WIDE), BF16)]
        + [packed(12, c1)] * 2,
        [pltpu.VMEM((2, 10, v, WIDE), BF16)],
        [*halo, partial, s_in, p_in, w_top, w_bottom],
    )
    halo = swap(near, far, "ty")
    (pre_in,) = call(
        skip_inner_kernel,
        "skip_inner",
        [((6, 8, c1, 256), F32)],
        [pltpu.VMEM((8, 10, c1, WIDE), BF16)],
        [s_in, s_out, gs1, ob1],
        flops=10**9,
    )
    (middle,) = call(
        middle_kernel,
        "middle",
        [((2, 4, c2, WIDE), BF16)],
        [pltpu.VMEM((4, 6, c1, WIDE), BF16)],
        [p_in, p_out, w2, b2],
        flops=5 * 10**8,
    )
    s2, p2, near, far = call(
        two_kernel,
        "two",
        [((6, 4, c2, WIDE), BF16), ((4, 2, c2, WIDE), BF16), packed(4, c2), packed(4, c2)],
        [pltpu.VMEM((10, 6, c1, WIDE), BF16)],
        [p_in, p_out, *halo, middle, g2, b2, pre_in],
    )
    halo = swap(near, far, "ty")
    pre2, near, far = call(
        skip_two_kernel,
        "skip_two",
        [((6, 4, c2, WIDE), F32), packed(8, c1), packed(8, c1)],
        [pltpu.VMEM((8, 6, c2, WIDE), BF16)],
        [s2, middle, s_out, gs2, ob2],
        flops=10**9,
    )
    skip_halo = swap(near, far, "ty")
    s3, coarse, c_send = call(
        three_kernel,
        "three",
        [((6, 2, c3, WIDE), BF16), ((c4, WIDE), BF16), packed(4, c4 // 4)],
        [pltpu.VMEM((8, 4, c2, WIDE), BF16), pltpu.VMEM((3, 3, c3, WIDE), BF16)],
        [p2, *halo, w3, b3, wc, bc],
    )
    halo = swap(c_send, c_send, "ty")
    (pre_out,) = call(
        skip_outer_kernel,
        "skip_outer",
        [((2, 8, c1, 256), F32)],
        [pltpu.VMEM((6, 10, c1, WIDE), BF16)],
        [s_in, s_out, *skip_halo, ws1, ob1],
        flops=5 * 10**8,
    )
    (pre3,) = call(
        skip_three_kernel,
        "skip_three",
        [((4, 2, c3, WIDE), F32)],
        [pltpu.VMEM((6, 4, c3, WIDE), BF16)],
        [s3, ws3, ob3],
        flops=10**9,
    )
    (back_two,) = call(
        back_kernel,
        "back",
        [((6, 4, c2, WIDE), BF16)],
        [pltpu.VMEM((3, 3, c4, WIDE), BF16), pltpu.VMEM((4, 4, c3, WIDE), BF16)],
        [coarse, *halo, pre3, pre2, wu3, wu2],
    )
    (back_one,) = call(
        last_kernel,
        "last",
        [((2, 8, c1, 1024), BF16)],
        [pltpu.VMEM((6, 6, c2, WIDE), BF16)],
        [back_two, pre_in, pre_out, wu1],
    )
    out = pl.pallas_call(
        head_kernel_body,
        name="head",
        out_shape=jax.ShapeDtypeStruct((2, v * 8, 1024), F32),
        in_specs=[pl.BlockSpec(memory_space=pltpu.VMEM)] * 4,
        out_specs=pl.BlockSpec(memory_space=pltpu.HBM),
        scratch_shapes=[
            pltpu.VMEM((2, v * 8, 1024), F32),
            pltpu.SemaphoreType.DMA((4,)),
        ],
        compiler_params=pltpu.CompilerParams(vmem_limit_bytes=16 * 2**20),
    )(x, back_one.reshape(2, 8 * c1, 1024), wh, bh)
    return out.reshape(2, v, 8, 1024)


def solution(mesh):
    return jax.shard_map(
        body,
        mesh=mesh,
        in_specs=(P(None, None, "ty", "tx"),) + (P(),) * 16,
        out_specs=P(None, None, "ty", "tx"),
        check_vma=False,
    )
```

```python
import jax
import jax.numpy as jnp
from jax import lax
from jax.experimental import pallas as pl
from jax.experimental.pallas import tpu as pltpu
from jax.sharding import PartitionSpec as P

LANES = 128
WIDE = 384
BF16 = jnp.bfloat16
F32 = jnp.float32


def swap(near_part, far_part, axis):
    size = lax.axis_size(axis)
    near = [(i, i ^ 1) for i in range(size)]
    far = [(i, (i + 1 if i % 2 else i - 1) % size) for i in range(size)]
    return lax.ppermute(near_part, axis, near), lax.ppermute(far_part, axis, far)


class Either:
    def __init__(self, cond, one, other):
        self.cond, self.one, self.other = cond, one, other

    def __getitem__(self, index):
        return jnp.where(self.cond, self.one[index], self.other[index])


def is_even(axis):
    return lax.axis_index(axis) % 2 == 0


def received(near, far, axis):
    even = is_even(axis)
    return Either(even, far, near), Either(even, near, far)


def pack_both(near, far, before, after):
    even = is_even("ty")
    pack(near, [jnp.where(even, b, a) for a, b in zip(before, after)])
    pack(far, [jnp.where(even, a, b) for a, b in zip(before, after)])


def call(body, name, out_shapes, scratch, args, limit=16, flops=0, aliases=None):
    specs = [pl.BlockSpec(memory_space=pltpu.VMEM)] * len(args)
    return pl.pallas_call(
        body,
        name=name,
        out_shape=[jax.ShapeDtypeStruct(s, d) for s, d in out_shapes],
        in_specs=specs,
        out_specs=[pl.BlockSpec(memory_space=pltpu.VMEM)] * len(out_shapes),
        scratch_shapes=scratch,
        input_output_aliases=aliases or {},
        cost_estimate=pl.CostEstimate(flops=flops, transcendentals=0, bytes_accessed=0),
        compiler_params=pltpu.CompilerParams(vmem_limit_bytes=limit * 2**20),
    )(*args)


def iota(shape, axis):
    return lax.broadcasted_iota(jnp.int32, shape, axis)


def edges():
    ty, tx = lax.axis_index("ty"), lax.axis_index("tx")
    ny, nx = lax.axis_size("ty"), lax.axis_size("tx")
    inside = (ty > 0, ty < ny - 1, tx > 0, tx < nx - 1)
    return [jnp.where(side, 1.0, 0.0) for side in inside]


def one_hot(cond):
    return jnp.where(cond, 1.0, 0.0).astype(BF16)


def dot(a, b):
    return jnp.dot(a, b, preferred_element_type=F32)


def silu(half):
    return half * (jnp.tanh(half) + 1.0)


def halved(weights):
    return (weights.astype(F32) * 0.5).astype(BF16)


def lane_mask(flags):
    lane = iota((1, WIDE), 1)
    place = lane & 15
    edge = lane >= 256
    left = jnp.where(edge & (place < 4), flags[2], 1.0)
    right = jnp.where(edge & (place >= 12), flags[3], 1.0)
    return left * right


def from_left(slab):
    lane = iota((1, LANES), 1)
    h0, h1, edge = slab[:, :128], slab[:, 128:256], slab[:, 256:]
    h0 = jnp.where(lane == 0, pltpu.roll(edge, 125, 1), pltpu.roll(h0, 1, 1))
    h1 = jnp.where(lane == 0, pltpu.roll(edge, 109, 1), pltpu.roll(h1, 1, 1))
    return jnp.concatenate([h0, h1, pltpu.roll(edge, 1, 1)], axis=1)


def from_right(slab):
    lane = iota((1, LANES), 1)
    h0, h1, edge = slab[:, :128], slab[:, 128:256], slab[:, 256:]
    h0 = jnp.where(lane == 127, pltpu.roll(edge, 115, 1), pltpu.roll(h0, 127, 1))
    h1 = jnp.where(lane == 127, pltpu.roll(edge, 99, 1), pltpu.roll(h1, 127, 1))
    return jnp.concatenate([h0, h1, pltpu.roll(edge, 127, 1)], axis=1)


def fill(scratch, row, slabs, valid=None):
    phases = len(slabs)
    for p, slab in enumerate(slabs):
        if valid is not None:
            slab = jnp.where(valid > 0.5, slab, jnp.zeros_like(slab))
        scratch[row, p + 1] = slab
        if p == 0:
            scratch[row, phases + 1] = from_right(slab)
        if p == phases - 1:
            scratch[row, 0] = from_left(slab)


def window(scratch, row, phase, rows, cols):
    v = scratch[pl.ds(row, rows), phase : phase + cols]
    return v.reshape(rows * cols * v.shape[2], v.shape[3])


def side(*parts):
    return jnp.concatenate(parts, axis=1)


def pack(out, slabs):
    lane = iota((1, LANES), 1)
    count = len(slabs)
    for n, slab in enumerate(slabs):
        out[2 * n] = slab[:, :128]
        out[2 * n + 1] = slab[:, 128:256]
    for g in range(0, count, 4):
        tile = slabs[g][:, 256:]
        for n in range(1, min(4, count - g)):
            tile = jnp.where(lane < 32 * n, tile, pltpu.roll(slabs[g + n][:, 256:], 32 * n, 1))
        out[2 * count + g // 4] = tile


def unpack(packed, n, count):
    tile = packed[2 * count + n // 4]
    if n % 4:
        tile = pltpu.roll(tile, 128 - 32 * (n % 4), 1)
    return side(packed[2 * n], packed[2 * n + 1], tile)


def tiles(count):
    return 2 * count + (count + 3) // 4


def turned(part):
    rows = part.shape[0]
    i, k = iota((rows, rows), 0), iota((rows, rows), 1)
    turn = one_hot(i == (k & 7) * (rows // 8) + (k >> 3))
    return dot(turn, part).astype(BF16)


def cols_kernel(x, near, far, _):
    lane = iota((1, LANES), 1)
    size = x.shape[1] // 4
    even = is_even("tx")
    for h in range(2):
        packed = []
        for start, first in ((0, 0), (896, 96)):
            tile = None
            for g in range(4):
                rows = slice(g * size, (g + 1) * size)
                piece = rolled(x[h, rows, start : start + 128], 32 * g - first)
                tile = piece if tile is None else jnp.where(lane < 32 * g, tile, piece)
            packed.append(tile)
        near[h] = jnp.where(even, packed[1], packed[0])
        far[h] = jnp.where(even, packed[0], packed[1])


def columns(packed, first):
    return jnp.concatenate([rolled(packed, first - 32 * g) for g in range(4)], axis=0)


def main_kernel(x, out):
    channels = x.shape[1] // 8
    lane = iota((1, LANES), 1)
    c = iota((1, 256), 1)
    split = one_hot(iota((256, 256), 0) == 8 * (c & 31) + (c >> 5))
    for h in range(2):
        blocks = [dot(x[h, :, q * 256 : (q + 1) * 256], split).astype(BF16) for q in range(4)]
        phases = []
        for p in range(8):
            half = slice((p // 4) * 128, (p // 4 + 1) * 128)
            tile = rolled(blocks[0][:, half], -32 * (p % 4))
            for q in range(1, 4):
                tile = jnp.where(lane < 32 * q, tile, rolled(blocks[q][:, half], 32 * (q - p % 4)))
            phases.append(tile)
        for q in range(4):
            part = turned(side(phases[2 * q], phases[2 * q + 1]))
            for r in range(8):
                rows = part[r * channels : (r + 1) * channels]
                for s in range(2):
                    out[r, 2 * q + s, :, h * 128 : (h + 1) * 128] = rows[:, s * 128 : (s + 1) * 128]


def rolled(value, shift):
    return pltpu.roll(value, shift % 128, 1) if shift % 128 else value


def ends_kernel(x, main, cols_near, cols_far, out, near, far):
    flags = edges()
    fl, fr = received(cols_near, cols_far, "tx")
    lane = iota((1, LANES), 1)
    channels = x.shape[1] // 8
    ends = []
    for h in range(2):
        before, after = columns(fl[h], 96), columns(fr[h], 0)
        a = jnp.where((lane >= 96) & (flags[2] > 0.5), before, jnp.where(lane < 32, x[h, :, :128], 0))
        b = jnp.where(lane >= 96, x[h, :, 896:], jnp.where((lane < 32) & (flags[3] > 0.5), after, 0))
        ends += [a.astype(BF16), b.astype(BF16)]
    ends = side(*ends)
    c = iota((1, 256), 1)
    row = 128 * ((c & 31) >> 3) + (((8 * (c & 7) + (c >> 5)) + 96) & 127)
    part = turned(dot(ends, one_hot(iota((512, 256), 0) == row)).astype(BF16))
    for r in range(8):
        rows = part[r * channels : (r + 1) * channels]
        for p in range(8):
            tile = rows[:, (p // 4) * 128 : (p // 4 + 1) * 128]
            out[r, p] = pltpu.roll(tile, 128 - 32 * (p % 4), 1) if p % 4 else tile
    pack_both(near, far, field_slabs(main, out, 0), field_slabs(main, out, 7))


def field_slabs(main, ends, r):
    return [side(main[r, p], ends[r, p]) for p in range(8)]


def conv_rows(xs, w, bias, row, q, group=1):
    rhs = side(*[window(xs, row, 2 * q + s, group + 2, 3) for s in range(2)])
    res = dot(w, rhs)
    size = bias.shape[0]
    return {
        (r, s): silu(res[r * size : (r + 1) * size, s * WIDE : (s + 1) * WIDE] + bias)
        for r in range(group)
        for s in range(2)
    }


def inner_kernel(main, ends, w, w_low, w_high, b, skip, pooled, outer, xs):
    flags = edges()
    for r in range(8):
        fill(xs, r, field_slabs(main, ends, r))
    mask = lane_mask(flags)
    bias = b[...]

    def one(k, carry):
        for q in range(4):
            for (r, s), y in conv_rows(xs, w[...], bias, 3 * k, q, 3).items():
                skip[3 * k + r, 2 * q + s] = (y * mask).astype(BF16)
        return carry

    lax.fori_loop(0, 2, one, 0)
    for k, (row, part) in enumerate(((0, w_low), (6, w_high))):
        for q in range(4):
            res = dot(part[...], side(*[window(xs, row, 2 * q + s, 2, 3) for s in range(2)]))
            for s in range(2):
                outer[k, 2 * q + s] = res[:, s * WIDE : (s + 1) * WIDE] + bias
    for k in range(2):
        for q in range(4):
            pooled[k, q] = mean([skip[2 * k + 1 + r, 2 * q + s] for r in range(2) for s in range(2)])


def mean(slabs):
    total = slabs[0].astype(F32)
    for slab in slabs[1:]:
        total = total + slab.astype(F32)
    return (total * 0.25).astype(BF16)


def outer_kernel(
    f_near, f_far, partial, skip_in, pooled_in, w_top, w_bottom, skip, pooled, near, far, xs
):
    flags = edges()
    above, below = received(f_near, f_far, "ty")
    fill(xs, 0, [unpack(above, p, 8) for p in range(8)], flags[0])
    fill(xs, 1, [unpack(below, p, 8) for p in range(8)], flags[1])
    mask = lane_mask(flags)
    for k, part in enumerate((w_top, w_bottom)):
        for q in range(4):
            res = dot(part[...], side(*[window(xs, k, 2 * q + s, 1, 3) for s in range(2)]))
            for s in range(2):
                y = silu(res[:, s * WIDE : (s + 1) * WIDE] + partial[k, 2 * q + s])
                skip[k, 2 * q + s] = (y * mask).astype(BF16)
    for q in range(4):
        pooled[0, q] = mean([src[0, 2 * q + s] for src in (skip, skip_in) for s in range(2)])
        ends = [skip_in[5, 2 * q + s] for s in range(2)] + [skip[1, 2 * q + s] for s in range(2)]
        pooled[1, q] = mean(ends)
    rows = [[ref[k, q] for q in range(4)] for ref, k in ((pooled, 0), (pooled_in, 0), (pooled_in, 1), (pooled, 1))]
    pack_both(near, far, rows[0] + rows[1] + rows[2], rows[1] + rows[2] + rows[3])


def middle_kernel(pooled_in, pooled, w2, b2, skip, xs):
    for n, (ref, r) in enumerate(((pooled, 0), (pooled_in, 0), (pooled_in, 1), (pooled, 1))):
        fill(xs, n, [ref[r, p] for p in range(4)])
    mask = lane_mask(edges())
    for q in range(2):
        for (r, s), y in conv_rows(xs, w2[...], b2[...], 0, q, 2).items():
            skip[r, 2 * q + s] = (y * mask).astype(BF16)


def two_kernel(pooled_in, pooled, p_near, p_far, middle, g2, b2, _, skip2, pooled2, near, far, xs):
    flags = edges()
    above, below = received(p_near, p_far, "ty")
    for r in range(3):
        fill(xs, r, [unpack(above, 4 * r + p, 12) for p in range(4)], flags[0])
        fill(xs, r + 5, [unpack(below, 4 * r + p, 12) for p in range(4)], flags[1])
    for n, (ref, r) in enumerate(((pooled, 0), (pooled_in, 0))):
        fill(xs, n + 3, [ref[r, p] for p in range(4)])
    for n, (ref, r) in enumerate(((pooled_in, 1), (pooled, 1))):
        fill(xs, n + 8, [ref[r, p] for p in range(4)])
    mask = lane_mask(flags)
    size = b2.shape[0]
    for k, first in ((0, 0), (1, 3)):
        rows = ((0, 1, 2, 3, 4), (8, 9, 5, 6, 7))[k]
        outside = mask * flags[k]
        for p in range(4):
            rhs = [window(xs, row, p, 1, 3) for row in rows]
            res = dot(g2[...], jnp.concatenate(rhs, axis=0))
            for r in range(3):
                inside = mask if r == (2, 0)[k] else outside
                y = silu(res[r * size : (r + 1) * size] + b2[...]) * inside
                skip2[first + r, p] = y.astype(BF16)
    order = [(skip2, 0), (skip2, 1), (skip2, 2), (middle, 0), (middle, 1), (skip2, 3), (skip2, 4), (skip2, 5)]
    for k in range(4):
        for q in range(2):
            pooled2[k, q] = mean([ref[r, 2 * q + s] for ref, r in order[2 * k : 2 * k + 2] for s in range(2)])
    before = [pooled2[r, p] for r in (2, 3) for p in range(2)]
    pack_both(near, far, before, [pooled2[r, p] for r in (0, 1) for p in range(2)])


def three_kernel(pooled2, q_near, q_far, w3, b3, wc, bc, skip3, coarse, send, xs, xc):
    flags = edges()
    above, below = received(q_near, q_far, "ty")
    for r in range(2):
        fill(xs, r, [unpack(above, 2 * r + p, 4) for p in range(2)], flags[0])
        fill(xs, r + 6, [unpack(below, 2 * r + p, 4) for p in range(2)], flags[1])
    for r in range(4):
        fill(xs, r + 2, [pooled2[r, p] for p in range(2)])
    mask = lane_mask(flags)
    for k in range(3):
        inside = mask * (flags[0] if k == 0 else flags[1]) if k != 1 else mask
        slabs = []
        for r in range(2):
            for (_, p), y in conv_rows(xs, w3[...], b3[...], 2 * k + r, 0).items():
                y = (y * inside).astype(BF16)
                skip3[2 * k + r, p] = y
                slabs.append(y)
        fill(xc, k, [mean(slabs)])
    res = silu(dot(wc[...], window(xc, 0, 0, 3, 3)) + bc[...])
    res = (res * mask).astype(BF16)
    coarse[...] = res
    size = res.shape[0] // 4
    pack(send, [res[n * size : (n + 1) * size] for n in range(4)])


def skip_three_kernel(s3, c, w, wu, b, out, xs, xc):
    fill(xc, 0, [c[...]])
    half = wu.shape[3] // 2
    for r in range(6):
        fill(xs, r, [s3[r, p] for p in range(2)])
    for r in range(4):
        res = dot(w[...], side(*[window(xs, r, p, 3, 3) for p in range(2)]))
        for p in range(2):
            start = half if r < 2 else 0
            own = dot(wu[1 - r % 2, p, :, start : start + half], window(xc, 0, p, 1, 2))
            out[r, p] = res[:, p * WIDE : (p + 1) * WIDE] + own + b[...]


def skip_two_kernel(s2, middle, s_out, w, b, out, near, far, xs):
    order = [(s2, 0), (s2, 1), (s2, 2), (middle, 0), (middle, 1), (s2, 3), (s2, 4), (s2, 5)]
    for n, (ref, r) in enumerate(order):
        fill(xs, n, [ref[r, p] for p in range(4)])
    bias = b[...]

    def pair(k, carry):
        for q in range(2):
            res = dot(w[...], side(*[window(xs, 2 * k, 2 * q + s, 4, 3) for s in range(2)]))
            for r in range(2):
                for s in range(2):
                    part = res[r * bias.shape[0] : (r + 1) * bias.shape[0]]
                    out[2 * k + r, 2 * q + s] = part[:, s * WIDE : (s + 1) * WIDE] + bias
        return carry

    lax.fori_loop(0, 3, pair, 0)
    pack_both(near, far, [s_out[0, p] for p in range(8)], [s_out[1, p] for p in range(8)])


def skip_inner_kernel(s_in, s_out, w, b, out, xs):
    fill(xs, 0, [s_out[0, p] for p in range(8)])
    for r in range(6):
        fill(xs, r + 1, [s_in[r, p] for p in range(8)])
    fill(xs, 7, [s_out[1, p] for p in range(8)])
    size = b.shape[0]
    for k in range(2):
        for p in range(8):
            res = dot(w[...], window(xs, 3 * k, p, 5, 3)[:, :256])
            for r in range(3):
                out[3 * k + r, p] = res[r * size : (r + 1) * size] + b[...]


def skip_outer_kernel(s_in, s_out, s_near, s_far, w, b, out, xs):
    flags = edges()
    above, below = received(s_near, s_far, "ty")
    fill(xs, 0, [unpack(above, p, 8) for p in range(8)], flags[0])
    for n, (ref, r) in enumerate(((s_out, 0), (s_in, 0), (s_in, 5), (s_out, 1))):
        fill(xs, n + 1, [ref[r, p] for p in range(8)])
    fill(xs, 5, [unpack(below, p, 8) for p in range(8)], flags[1])
    for k in range(2):
        for p in range(8):
            out[k, p] = dot(w[...], window(xs, 3 * k, p, 3, 3)[:, :256]) + b[...]


def back_kernel(c_near, c_far, pre3, pre2, wu3, wu2, out, xc, xb):
    flags = edges()
    above, below = received(c_near, c_far, "ty")
    halo = lambda packed: [jnp.concatenate([unpack(packed, n, 4) for n in range(4)], axis=0)]
    fill(xc, 0, halo(above), flags[0])
    fill(xc, 1, halo(below), flags[1])
    mask = lane_mask(flags)
    half = wu3.shape[3] // 2
    slabs = {}
    for r in range(4):
        start = 0 if r < 2 else half
        for p in range(2):
            res = dot(wu3[1 - r % 2, p, :, start : start + half], window(xc, r // 2, p, 1, 2))
            inside = mask * flags[0] if r == 0 else mask * flags[1] if r == 3 else mask
            slabs[r, p] = (silu(res + pre3[r, p]) * inside).astype(BF16)
    for r in range(4):
        fill(xb, r, [slabs[r, p] for p in range(2)])

    def pair(k, carry):
        for b in range(2):
            rhs = side(*[window(xb, k, (p + 1) // 2, 2, 2) for p in (b, b + 2)])
            res = dot(wu2[b], rhs)
            size = res.shape[0] // 2
            for i in range(2):
                valid = jnp.where(
                    (k == 0) & (i == 0), flags[0], jnp.where((k == 2) & (i == 1), flags[1], 1.0)
                )
                inside = mask * valid
                rows = res[i * size : (i + 1) * size]
                for n in range(2):
                    y = silu(rows[:, n * WIDE : (n + 1) * WIDE] + pre2[2 * k + i, b + 2 * n])
                    out[2 * k + i, b + 2 * n] = (y * inside).astype(BF16)
        return carry

    lax.fori_loop(0, 3, pair, 0)


def last_kernel(bt, pre_in, pre_out, wu, out, xb):
    for r in range(6):
        fill(xb, r, [bt[r, p] for p in range(4)])
    size = wu.shape[0] // 4
    for k in range(5):
        for m in range(5):
            res = dot(wu[...], window(xb, k, m, 2, 2)[:, :256])
            for i in range(2):
                for j in range(2):
                    r, p = 2 * k - 1 + i, 2 * m - 1 + j
                    if not (0 <= r < 8 and 0 <= p < 8):
                        continue
                    pre = pre_out[0, p] if r == 0 else pre_out[1, p] if r == 7 else pre_in[r - 1, p]
                    n = 2 * (1 - i) + 1 - j
                    y = silu(res[n * size : (n + 1) * size] + pre).astype(BF16)
                    for h in range(2):
                        lanes = slice(h * 128, (h + 1) * 128)
                        out[h, r, :, p * 128 : (p + 1) * 128] = y[:, lanes]


def head_kernel_body(fields, back, w, offset, out, buf, sems):
    lane = iota((1, LANES), 1)
    c = iota((1, 256), 1)
    merge = one_hot(iota((256, 256), 0) == 32 * (c & 7) + (c >> 3))
    copies = []
    for h in range(2):
        for half in range(2):
            blocks = []
            for q in (2 * half, 2 * half + 1):
                pieces = []
                for g in range(2):
                    tile = rolled(back[h, :, g * 512 : g * 512 + 128], -32 * q)
                    for n in range(1, 4):
                        start = g * 512 + n * 128
                        piece = rolled(back[h, :, start : start + 128], 32 * (n - q))
                        tile = jnp.where(lane < 32 * n, tile, piece)
                    pieces.append(tile)
                blocks.append(dot(side(*pieces), merge).astype(BF16))
            cols = slice(half * 512, (half + 1) * 512)
            base = fields[h, :, cols].astype(F32) + side(offset[...], offset[...])
            buf[h, :, cols] = base + dot(w[...], side(*blocks))
            n = 2 * h + half
            copies.append(pltpu.make_async_copy(buf.at[h, :, cols], out.at[h, :, cols], sems.at[n]))
            copies[n].start()
    for copy in copies:
        copy.wait()


def flip(value):
    eye = one_hot(iota((value.shape[1],) * 2, 0) == iota((value.shape[1],) * 2, 1))
    dims = (((1,), (1,)), ((), ()))
    return lax.dot_general(eye, value, dims, preferred_element_type=F32).astype(BF16)


def column(row, width, repeat=1):
    size = row.shape[1]
    i, j = iota((size * repeat, size), 0), iota((size * repeat, size), 1)
    col = jnp.sum(jnp.where(i // repeat == j, row, 0.0), axis=1, keepdims=True)
    return jnp.broadcast_to(col, (size * repeat, width))


def sums(a):
    return ((0,), (1, 2)) if a == 0 else ((0, 1), (2,))


def summed(tap, a, b, i, j):
    total = None
    for dy in sums(a)[i]:
        for dx in sums(b)[j]:
            value = tap(dy, dx).astype(F32)
            total = value if total is None else total + value
    return (total * 0.5).astype(BF16)


def placed(parts, width):
    size = parts[0].shape[1]
    total = None
    for n, part in enumerate(parts):
        spot = one_hot(iota((size, width), 1) == iota((size, width), 0) + n * size)
        value = dot(part, spot)
        total = value if total is None else total + value
    return total.astype(BF16)


def grouped(w, rows):
    size, step = w.shape[1], w.shape[1] // 3
    width = step * (rows + 2)
    i, j = iota((size, width), 0), iota((size, width), 1)
    parts = [dot(w, one_hot(j == i + n * step)).astype(BF16) for n in range(rows)]
    return jnp.concatenate(parts, axis=0)


NINE = [(dy, dx) for dy in range(3) for dx in range(3)]
FOUR = [(i, j) for i in range(2) for j in range(2)]


def early_kernel(k1, k2, k3, r1, r2, r3, g1, low, high, top, bottom, w2, g2, w3, b1, b2, b3):
    w1 = halved(placed([k1[n] for n in NINE], 9 * k1.shape[3]))
    step = 3 * k1.shape[3]
    g1[...] = grouped(w1, 3)
    for ref, start in ((low, step), (high, 0), (top, 0), (bottom, 2 * step)):
        i, j = iota((w1.shape[1], ref.shape[1]), 0), iota((w1.shape[1], ref.shape[1]), 1)
        ref[...] = dot(w1, one_hot(i == j + start)).astype(BF16)
    flat = halved(flip(k2[...].reshape(-1, k2.shape[3])))
    w2[...] = grouped(flat, 2)
    g2[...] = grouped(flat, 3)
    w3[...] = halved(flip(k3[...].reshape(-1, k3.shape[3])))
    for r, b in ((r1, b1), (r2, b2), (r3, b3)):
        b[...] = column(r[...] * 0.5, WIDE)


def late_kernel(
    kc, d3, d2, d1, hk, rc, r3, r2, r1, rh, wc, wu3, ws3, wu2, gs2, wu1, ws1, gs1, wh, bc, b3, b2, b1, bh
):
    wc[...] = halved(flip(kc[...].reshape(-1, kc.shape[3])))
    for r, b in ((rc, bc), (r3, b3), (r2, b2), (r1, b1)):
        b[...] = column(r[...] * 0.5, b.shape[1])
    bh[...] = column(rh[...], bh.shape[1], 8)
    up3, up2, up1 = wu3.shape[3] // 4, wu2.shape[2] // 4, wu1.shape[1] // 4
    n2, n1 = d2.shape[2], d1.shape[2]
    for a in range(2):
        for b in range(2):
            tall = [summed(lambda y, x: d3[y, x, :up3, :], a, b, i, j) for i, j in FOUR]
            wu3[a, b] = flip(jnp.concatenate(tall, axis=0))
            wide = [summed(lambda y, x: d2[y, x, :, :up2], a, b, i, j) for i, j in FOUR]
            wu2[b, (1 - a) * n2 : (2 - a) * n2] = jnp.concatenate(wide, axis=1)
            wide = [summed(lambda y, x: d1[y, x, :, :up1], a, b, i, j) for i, j in FOUR]
            wu1[(2 * a + b) * n1 : (2 * a + b + 1) * n1] = placed(wide, wu1.shape[1])
    ws3[...] = halved(flip(jnp.concatenate([d3[y, x, up3:, :] for y, x in NINE], axis=0)))
    skips = [halved(d2[y, x, :, up2:]) for y, x in NINE]
    gs2[...] = grouped(placed(skips, 9 * skips[0].shape[1]), 2)
    ws1[...] = halved(placed([d1[y, x, :, up1:] for y, x in NINE], ws1.shape[1]))
    gs1[...] = grouped(ws1[...], 3)
    v, c = hk.shape[1], hk.shape[0]
    spread = one_hot(iota((v * 8, v), 0) // 8 == iota((v * 8, v), 1))
    dims = (((1,), (1,)), ((), ()))
    tall = lax.dot_general(spread, hk[...], dims, preferred_element_type=F32).astype(BF16)
    i, k = iota((v * 8, 8 * c), 0), iota((v * 8, 8 * c), 1)
    tiled = dot(tall, one_hot(iota((c, 8 * c), 0) == iota((c, 8 * c), 1) % c))
    wh[...] = jnp.where(i % 8 == k // c, tiled, 0.0).astype(BF16)


def body(
    fields,
    kernel_one,
    bias_one,
    kernel_two,
    bias_two,
    kernel_three,
    bias_three,
    kernel_coarse,
    bias_coarse,
    decode_three,
    offset_three,
    decode_two,
    offset_two,
    decode_one,
    offset_one,
    head_kernel,
    head_offset,
):
    c1, c2, c3, c4 = (k.shape[3] for k in (kernel_one, kernel_two, kernel_three, kernel_coarse))
    v = fields.shape[1]

    x = fields.reshape(2, v * 8, 1024)
    near, far, x = call(
        cols_kernel,
        "cols",
        [((2, 2 * v, LANES), BF16)] * 2 + [(x.shape, BF16)],
        [],
        [x],
        aliases={0: 2},
    )
    cols = swap(near, far, "tx")

    row = lambda bias: bias[None, :]
    turn = lambda kernel: jnp.transpose(kernel, (0, 1, 3, 2))
    weights = lambda *shape: (shape, BF16)
    biases = lambda size, width=WIDE: ((size, width), F32)
    g1, w_low, w_high, w_top, w_bottom, w2, g2, w3, b1, b2, b3 = call(
        early_kernel,
        "early",
        [weights(3 * c1, 15 * v)]
        + [weights(c1, rows * 3 * v) for rows in (2, 2, 1, 1)]
        + [weights(2 * c2, 12 * c1), weights(3 * c2, 15 * c1), weights(c3, 9 * c2)]
        + [biases(c1), biases(c2), biases(c3)],
        [],
        [turn(kernel_one), kernel_two, kernel_three, row(bias_one), row(bias_two), row(bias_three)],
    )
    wc, wu3, ws3, wu2, gs2, wu1, ws1, gs1, wh, bc, ob3, ob2, ob1, bh = call(
        late_kernel,
        "late",
        [weights(c4, 9 * c3), weights(2, 2, c3, 4 * c4), weights(c3, 9 * c3)]
        + [weights(2, 2 * c2, 4 * c3), weights(2 * c2, 12 * c2)]
        + [weights(4 * c1, 4 * c2), weights(c1, 9 * c1), weights(3 * c1, 15 * c1)]
        + [weights(8 * v, 8 * c1)]
        + [biases(c4), biases(c3), biases(c2), biases(c1, 256), biases(8 * v, 256)],
        [],
        [kernel_coarse, decode_three, turn(decode_two), turn(decode_one), head_kernel]
        + [row(b) for b in (bias_coarse, offset_three, offset_two, offset_one, head_offset)],
        flops=5 * 10**8,
    )
    (main,) = call(main_kernel, "main", [((8, 8, v, 256), BF16)], [], [x], flops=10**9)
    packed = lambda count, size: ((tiles(count), size, LANES), BF16)
    ends, near, far = call(
        ends_kernel,
        "ends",
        [((8, 8, v, LANES), BF16), packed(8, v), packed(8, v)],
        [],
        [x, main, *cols],
    )
    halo = swap(near, far, "ty")
    s_in, p_in, partial = call(
        inner_kernel,
        "inner",
        [((6, 8, c1, WIDE), BF16), ((2, 4, c1, WIDE), BF16), ((2, 8, c1, WIDE), F32)],
        [pltpu.VMEM((8, 10, v, WIDE), BF16)],
        [main, ends, g1, w_low, w_high, b1],
        flops=10**9,
    )
    s_out, p_out, near, far = call(
        outer_kernel,
        "outer",
        [((2, 8, c1, WIDE), BF16), ((2, 4, c1, WIDE), BF16)]
        + [packed(12, c1)] * 2,
        [pltpu.VMEM((2, 10, v, WIDE), BF16)],
        [*halo, partial, s_in, p_in, w_top, w_bottom],
    )
    halo = swap(near, far, "ty")
    (pre_in,) = call(
        skip_inner_kernel,
        "skip_inner",
        [((6, 8, c1, 256), F32)],
        [pltpu.VMEM((8, 10, c1, WIDE), BF16)],
        [s_in, s_out, gs1, ob1],
        flops=10**9,
    )
    (middle,) = call(
        middle_kernel,
        "middle",
        [((2, 4, c2, WIDE), BF16)],
        [pltpu.VMEM((4, 6, c1, WIDE), BF16)],
        [p_in, p_out, w2, b2],
        flops=5 * 10**8,
    )
    s2, p2, near, far = call(
        two_kernel,
        "two",
        [((6, 4, c2, WIDE), BF16), ((4, 2, c2, WIDE), BF16), packed(4, c2), packed(4, c2)],
        [pltpu.VMEM((10, 6, c1, WIDE), BF16)],
        [p_in, p_out, *halo, middle, g2, b2, pre_in],
    )
    halo = swap(near, far, "ty")
    pre2, near, far = call(
        skip_two_kernel,
        "skip_two",
        [((6, 4, c2, WIDE), F32), packed(8, c1), packed(8, c1)],
        [pltpu.VMEM((8, 6, c2, WIDE), BF16)],
        [s2, middle, s_out, gs2, ob2],
        flops=10**9,
    )
    skip_halo = swap(near, far, "ty")
    s3, coarse, c_send = call(
        three_kernel,
        "three",
        [((6, 2, c3, WIDE), BF16), ((c4, WIDE), BF16), packed(4, c4 // 4)],
        [pltpu.VMEM((8, 4, c2, WIDE), BF16), pltpu.VMEM((3, 3, c3, WIDE), BF16)],
        [p2, *halo, w3, b3, wc, bc],
    )
    halo = swap(c_send, c_send, "ty")
    (pre_out,) = call(
        skip_outer_kernel,
        "skip_outer",
        [((2, 8, c1, 256), F32)],
        [pltpu.VMEM((6, 10, c1, WIDE), BF16)],
        [s_in, s_out, *skip_halo, ws1, ob1],
        flops=5 * 10**8,
    )
    (pre3,) = call(
        skip_three_kernel,
        "skip_three",
        [((4, 2, c3, WIDE), F32)],
        [pltpu.VMEM((6, 4, c3, WIDE), BF16), pltpu.VMEM((1, 3, c4, WIDE), BF16)],
        [s3, coarse, ws3, wu3, ob3],
        flops=10**9,
    )
    (back_two,) = call(
        back_kernel,
        "back",
        [((6, 4, c2, WIDE), BF16)],
        [pltpu.VMEM((2, 3, c4, WIDE), BF16), pltpu.VMEM((4, 4, c3, WIDE), BF16)],
        [*halo, pre3, pre2, wu3, wu2],
    )
    (back_one,) = call(
        last_kernel,
        "last",
        [((2, 8, c1, 1024), BF16)],
        [pltpu.VMEM((6, 6, c2, WIDE), BF16)],
        [back_two, pre_in, pre_out, wu1],
    )
    out = pl.pallas_call(
        head_kernel_body,
        name="head",
        out_shape=jax.ShapeDtypeStruct((2, v * 8, 1024), F32),
        in_specs=[pl.BlockSpec(memory_space=pltpu.VMEM)] * 4,
        out_specs=pl.BlockSpec(memory_space=pltpu.HBM),
        scratch_shapes=[
            pltpu.VMEM((2, v * 8, 1024), F32),
            pltpu.SemaphoreType.DMA((4,)),
        ],
        compiler_params=pltpu.CompilerParams(vmem_limit_bytes=16 * 2**20),
    )(x, back_one.reshape(2, 8 * c1, 1024), wh, bh)
    return out.reshape(2, v, 8, 1024)


def solution(mesh):
    return jax.shard_map(
        body,
        mesh=mesh,
        in_specs=(P(None, None, "ty", "tx"),) + (P(),) * 16,
        out_specs=P(None, None, "ty", "tx"),
        check_vma=False,
    )
```
